768 devices in a mesh: band: 32 (over x, y), field: 24 (over z, core).
Axes of the slice: x: 4, y: 8, z: 12, core: 2. Of those that a mesh axis runs over, the one named last changes fastest.
Arguments:
- fourier: bfloat16 [768, 192, 1792], P(None, 'field', 'band'), may hold values from -6 to 6
- quad_weights: float32 [1792], P('band'), may hold values from 0.1 to 1.9
- legendre: bfloat16 [768, 1792, 768], P(('band', 'field')), may hold values from -0.125 to 0.125
- slot_wave: int32 [768], replicated, may hold values from 0 to 767, each once
- vert_proj: float32 [96, 96], replicated, may hold values from -0.625 to 0.625
- vert_recon: float32 [96, 96], replicated, may hold values from -0.625 to 0.625
- vert_rates: float32 [96], replicated, may hold values from 0.3 to 30
Outputs:
- spectral: bfloat16 [768, 2, 96, 768], P(('band', 'field'))
- returned: bfloat16 [768, 192, 1792], P(None, 'field', 'band')
The draws below stay inside these ranges and needn't reach their ends.
Inputs may be any that keep to these rules, and one draw needn't show every extreme that they name: `slot_wave`: every wavenumber 0 .. 767 stands in exactly one slot.
All inputs are finite; a program needn't handle non-finite values.
Results may differ from the reference program's by a relative error of at most 0.0056.
Values may be sent and summed in bfloat16 or wider, within the bound.
A program may use at most 32 MiB of HBM per device.

```python
import math
import jax
import jax.numpy as jnp
from jax import lax

LEV = 96
T_SIZE = 768
NLAT = 1792


def block_scale(key, extent, cuts, least, top_value):
    def one(dim, parts):
        heights = jax.random.uniform(jax.random.fold_in(jax.random.fold_in(key, 6), dim), (parts,), jnp.float32, least / len(cuts), top_value / len(cuts))
        return jnp.repeat(jnp.exp(heights), extent[dim] // parts).reshape((-1,) + (1,) * (len(extent) - dim - 1))

    factor_of = one(*cuts[0])
    for cut in cuts[1:]:
        factor_of = factor_of * one(*cut)
    return factor_of


def bell_draw(own_key, dims, deviation, reach, cuts=(), held_as=jnp.bfloat16):
    loudness = block_scale(own_key, dims, cuts, -0.22, 0.18) if cuts else 1.0
    drawn = jax.random.normal(own_key, dims, jnp.float32) * deviation * loudness
    return jnp.minimum(jnp.maximum(drawn, -reach), reach).astype(held_as)


def setup_inputs(seed: int = 0) -> dict:
    splits = jax.random.split(jax.random.key(seed), 8)
    fourier = bell_draw(splits[0], (T_SIZE, 2 * LEV, NLAT), 1.0, 6.0, ((1, 24), (2, 32)))
    quad_weights = jnp.clip(1.0 + 0.18 * jax.random.normal(splits[1], (NLAT,), jnp.float32), 0.1, 1.9)
    legendre = bell_draw(splits[2], (T_SIZE, NLAT, T_SIZE), NLAT ** -0.5, 0.125, ((0, 768),))
    slot_wave = jax.random.permutation(splits[3], T_SIZE).astype(jnp.int32)
    vert_proj = bell_draw(splits[4], (LEV, LEV), LEV ** -0.5, 0.625, (), jnp.float32)
    vert_recon = bell_draw(splits[5], (LEV, LEV), LEV ** -0.5, 0.625, (), jnp.float32)
    vert_rates = jnp.clip(jnp.exp(jax.random.uniform(splits[6], (LEV,), jnp.float32, math.log(0.3), math.log(30.0))), 0.3, 30.0)
    return dict(fourier=fourier, quad_weights=quad_weights, legendre=legendre, slot_wave=slot_wave, vert_proj=vert_proj, vert_recon=vert_recon, vert_rates=vert_rates)


def damping(vert_rates, total):
    order = jnp.arange(total).astype(jnp.float32)
    growth = order * (order + 1.0) / float(total * total)
    return 1.0 / (1.0 + vert_rates[:, None] * growth[None, :])


def reference(fourier, quad_weights, legendre, slot_wave, vert_proj, vert_recon, vert_rates):
    weighted = (fourier.astype(jnp.float32) * quad_weights).astype(jnp.bfloat16)
    gamma = damping(vert_rates, T_SIZE)
    degree = jnp.arange(T_SIZE).astype(jnp.int32)

    def one_slot(items):
        table, wave = items
        data = weighted[wave]
        direct = jnp.dot(data, table, preferred_element_type=jnp.float32).reshape(2, LEV, T_SIZE)
        modes = jnp.einsum("jl,cln->cjn", vert_proj, direct, precision=lax.Precision.HIGHEST) * gamma
        solved = jnp.einsum("lj,cjn->cln", vert_recon, modes, precision=lax.Precision.HIGHEST)
        keep = (degree >= wave).astype(jnp.float32)
        spectral_one = (solved * keep).astype(jnp.bfloat16)
        back = lax.dot_general(spectral_one.reshape(2 * LEV, T_SIZE), table, (((1,), (1,)), ((), ())),
                               preferred_element_type=jnp.float32)
        return spectral_one, back.astype(jnp.bfloat16)

    spectral, backs = lax.map(one_slot, (legendre, slot_wave.astype(jnp.int32)))
    inverse = jnp.zeros((T_SIZE,), jnp.int32).at[slot_wave].set(jnp.arange(T_SIZE).astype(jnp.int32))
    return spectral, backs[inverse]
```

```python
import functools

import jax
import jax.numpy as jnp
from jax import lax
from jax.experimental import pallas as pl
from jax.experimental.pallas import tpu as pltpu
from jax.sharding import PartitionSpec as P

MESH = pl.DeviceIdType.MESH
F32, BF16 = jnp.float32, jnp.bfloat16
LEV = 96
NX, NY, NZ = 4, 8, 12
NB, NF = NX * NY, 2 * NZ
HB = NB // 2
LATS = 56
PAIR = 2 * LATS
TAIL = 128 - PAIR
ND = HB // 2 - 1
Z_ORDER = (6, 5, -5, 4, -4, 3, -3, 2, -2, 1, -1, 0)
Y_ORDER = (4, 3, -3, 2, -2, 1, -1, 0)


def band_of(parity, j):
    return (parity + 2 * (j // NY)) * NY + j % NY


def lanes():
    return lax.broadcasted_iota(jnp.int32, (8, 128), 1)


def roll(v, by):
    return pltpu.roll(v, by % 128, 1)


def dense_to_pair(src, dst, z):
    lane = lanes()
    low = lane < LATS
    halves = []
    for core in range(2):
        f = 2 * z + core
        tiles = [src[f, i].astype(F32) for i in range(ND)]
        last = roll(tiles[0], TAIL)
        for i in range(1, ND):
            last = jnp.where(lane < TAIL * i, last, roll(tiles[i], TAIL + TAIL * i))
        halves.append(tiles + [last])
    for i in range(ND + 1):
        one, two = halves[0][i], halves[1][i]
        dst[2 * i, z] = jnp.where(low, one, roll(two, LATS)).astype(BF16)
        dst[2 * i + 1, z] = jnp.where(low, roll(one, -LATS), two).astype(BF16)


def pair_to_dense(src, z):
    lane = lanes()
    low, body = lane < LATS, lane < PAIR
    first, second = [], []
    for i in range(ND + 1):
        even, odd = src[2 * i, z].astype(F32), src[2 * i + 1, z].astype(F32)
        first.append(jnp.where(low, even, roll(odd, LATS)))
        second.append(jnp.where(low, roll(even, -LATS), odd))
    out = []
    for tiles in (first, second):
        out.append([jnp.where(body, tiles[i], roll(tiles[ND], PAIR - TAIL * i)) for i in range(ND)])
    return out


def exchange_kernel(
    waves, quad, rates, proj, recon, fourier_hbm, legendre_hbm,
    spectral, last_a, last_b,
    fourier, legendre, left, direct,
    sa1, ra1, sa2, ra2, sb1, rb1, sb2, rb2,
    xa, ya, za, xb, yb, zb, vb,
    local_sem, send_sem, recv_sem,
):
    b, f = lax.axis_index("band"), lax.axis_index("field")
    x, y = b // NY, lax.rem(b, NY)
    z, core = f // 2, lax.rem(f, 2)
    parity, mine = lax.rem(x, 2), (x // 2) * NY + y

    barrier = pltpu.get_barrier_semaphore()

    def greet_band(i, carry):
        pl.semaphore_signal(barrier, 1, device_id=(lax.rem(b + i, NB), f), device_id_type=MESH)
        return carry

    def greet_field(i, carry):
        pl.semaphore_signal(barrier, 1, device_id=(b, lax.rem(f + i, NF)), device_id_type=MESH)
        return carry

    lax.fori_loop(1, NF, greet_field, 0)
    lax.fori_loop(1, NB, greet_band, 0)

    fetch = pltpu.make_async_copy(fourier_hbm, fourier, local_sem.at[0])
    fetch.start()
    table = []
    for part in range(2):
        side = parity if part == 0 else 1 - parity
        tail_at = band_of(side, HB - 2) * LATS
        for i in range(ND):
            row = (part * ND + i) * 128
            at = pl.multiple_of(band_of(side, 2 * i) * LATS, 16)
            table.append(pltpu.make_async_copy(
                legendre_hbm.at[0, pl.ds(at, PAIR)], legendre.at[pl.ds(row, PAIR)], local_sem.at[1]))
            at = pl.multiple_of(tail_at + TAIL * i, 16)
            table.append(pltpu.make_async_copy(
                legendre_hbm.at[0, pl.ds(at, TAIL)], legendre.at[pl.ds(row + PAIR, TAIL)], local_sem.at[1]))
    for copy in table:
        copy.start()
    fetch.wait()

    weight = quad[...]

    def picked(band, field):
        wave = waves[band * NF + field]
        return fourier[wave].astype(F32) * weight

    def pack_dense(field, carry):
        pieces = [picked(band_of(parity, j), field) for j in range(HB)]
        last = jnp.concatenate(pieces[HB - 2:], axis=1)
        for i in range(ND):
            tail = last[:, TAIL * i:TAIL * (i + 1)]
            tile = jnp.concatenate([pieces[2 * i], pieces[2 * i + 1], tail], axis=1)
            sa1[field, i] = tile.astype(BF16)
        return carry

    lax.fori_loop(0, NF, pack_dense, 0)
    empty = jnp.zeros((8, TAIL), F32)

    def pack_pair(j, carry):
        band = (1 - parity + 2 * (j // NY)) * NY + lax.rem(j, NY)
        for k in range(NZ):
            tile = jnp.concatenate([picked(band, 2 * k), picked(band, 2 * k + 1), empty], axis=1)
            sb1[j, k] = tile.astype(BF16)
        return carry

    lax.fori_loop(0, HB, pack_pair, 0)
    pl.semaphore_wait(barrier, NB + NF - 2)

    def send(src, dst, phase, device):
        pltpu.make_async_remote_copy(
            src_ref=src, dst_ref=dst, send_sem=send_sem.at[phase], recv_sem=recv_sem.at[phase],
            device_id=device, device_id_type=MESH).start()

    def send_field(src, dst, phase):
        for d in Z_ORDER:
            for k in range(2):
                if d == 0 and k == 0:
                    continue
                to = lax.rem(z + d + NZ, NZ) * 2 + lax.rem(core + k, 2)
                send(src.at[to], dst.at[f], phase, (b, to))

    def send_band(src, dst, phase, same):
        steps = (2, 0) if same else (1, 3)
        for dy in Y_ORDER:
            for dx in steps:
                if dx == 0 and dy == 0:
                    continue
                to_x, to_y = lax.rem(x + dx, NX), lax.rem(y + dy + NY, NY)
                to = (to_x // 2) * NY + to_y
                send(src.at[to], dst.at[mine], phase, (to_x * NY + to_y, f))

    def wait_all(ref, phase, count, received):
        some = ref.at[pl.ds(0, count)]
        copy = pltpu.make_async_remote_copy(
            src_ref=some, dst_ref=some, send_sem=send_sem.at[phase], recv_sem=recv_sem.at[phase],
            device_id=(b, f), device_id_type=MESH)
        if received:
            copy.wait_recv()
        else:
            copy.wait_send()

    def over_z(body):
        def step(k, carry):
            body(k)
            return carry

        lax.fori_loop(0, NZ, step, 0)

    def put_dense(src, dst):
        def body(k):
            out = pair_to_dense(src, k)
            for c in range(2):
                for i in range(ND):
                    dst[2 * k + c, i] = out[c][i].astype(BF16)

        over_z(body)

    send_field(sa1, ra1, 0)
    send_band(sb1, rb1, 1, False)
    ra1[f] = sa1[f]

    wait_all(rb1, 1, HB, True)
    put_dense(rb1, sb2)
    send_field(sb2, rb2, 2)
    rb2[f] = sb2[f]

    wait_all(ra1, 0, NF - 1, True)
    over_z(functools.partial(dense_to_pair, ra1, sa2))
    send_band(sa2, ra2, 3, True)
    ra2[mine] = sa2[mine]

    for copy in table:
        copy.wait()
    total = spectral.shape[1]
    step_n = 256
    half_k = ND * 128

    wait_all(ra2, 3, HB - 1, True)

    def left_a(k):
        out = pair_to_dense(ra2, k)
        for i in range(ND):
            both = jnp.concatenate([out[0][i], out[1][i]], axis=0)
            left[pl.ds(pl.multiple_of(16 * k, 16), 16), 128 * i:128 * (i + 1)] = both.astype(BF16)

    over_z(left_a)
    for n in range(0, total, step_n):
        direct[:, n:n + step_n] = jnp.dot(
            left[:, :half_k], legendre[:half_k, n:n + step_n], preferred_element_type=F32)

    wait_all(rb2, 2, NF - 1, True)

    def left_b(k):
        for i in range(ND):
            both = jnp.concatenate([rb2[2 * k, i].astype(F32), rb2[2 * k + 1, i].astype(F32)], axis=0)
            left[pl.ds(pl.multiple_of(16 * k, 16), 16), half_k + 128 * i:half_k + 128 * (i + 1)] = both.astype(BF16)

    over_z(left_b)
    my_wave = waves[b * NF + f]
    for n in range(0, total, step_n):
        part = direct[:, n:n + step_n] + jnp.dot(
            left[:, half_k:], legendre[half_k:, n:n + step_n], preferred_element_type=F32)
        order = (lax.broadcasted_iota(jnp.int32, (LEV, step_n), 1) + n).astype(F32)
        gamma = 1.0 / (1.0 + rates[...] * (order * (order + 1.0) / float(total * total)))
        degree = lax.broadcasted_iota(jnp.int32, (LEV, step_n), 1) + n
        for c in range(2):
            modes = gamma * jnp.dot(
                proj[...], part[LEV * c:LEV * (c + 1)], precision=lax.Precision.HIGHEST, preferred_element_type=F32)
            solved = jnp.dot(recon[...], modes, precision=lax.Precision.HIGHEST, preferred_element_type=F32)
            kept = jnp.where(degree >= my_wave, solved, 0.0)
            spectral[LEV * c:LEV * (c + 1), n:n + step_n] = kept.astype(BF16)

    def back(part, out):
        for i in range(ND):
            row = (part * ND + i) * 128
            made = lax.dot_general(
                spectral[...], legendre[row:row + 128, :], (((1,), (1,)), ((), ())), preferred_element_type=F32)
            out[:, i] = made.reshape(NF, 8, 128).astype(BF16)

    back(0, xa)
    send_field(xa, ya, 4)
    ya[f] = xa[f]
    back(1, xb)
    over_z(functools.partial(dense_to_pair, xb, yb))
    send_band(yb, zb, 5, False)

    wait_all(zb, 5, HB, True)
    put_dense(zb, vb)
    send_field(vb, last_b, 6)
    last_b[f] = vb[f]

    wait_all(ya, 4, NF - 1, True)
    over_z(functools.partial(dense_to_pair, ya, za))
    send_band(za, last_a, 7, True)
    last_a[mine] = za[mine]

    wait_all(last_a, 7, HB - 1, True)
    wait_all(last_b, 6, NF - 1, True)
    for ref, phase, count in (
        (sa1, 0, NF - 1), (sb1, 1, HB), (sb2, 2, NF - 1), (sa2, 3, HB - 1),
        (xa, 4, NF - 1), (yb, 5, HB), (vb, 6, NF - 1), (za, 7, HB - 1),
    ):
        wait_all(ref, phase, count, False)


def place_kernel(waves, from_a, from_b, returned):
    b = lax.axis_index("band")
    parity = lax.rem(b // NY, 2)
    lane = lanes()

    def put(band, field, tile):
        returned[waves[band * NF + field]] = tile[:, :LATS].astype(BF16)

    def one_a(j, carry):
        band = (parity + 2 * (j // NY)) * NY + lax.rem(j, NY)
        for k in range(NZ):
            tile = from_a[j, k].astype(F32)
            put(band, 2 * k, tile)
            put(band, 2 * k + 1, roll(tile, -LATS))
        return carry

    lax.fori_loop(0, HB, one_a, 0)

    def one_b(field, carry):
        tiles = [from_b[field, i].astype(F32) for i in range(ND)]
        last = roll(tiles[0], TAIL)
        for i in range(1, ND):
            last = jnp.where(lane < TAIL * i, last, roll(tiles[i], TAIL + TAIL * i))
        for i, tile in enumerate(tiles + [last]):
            put(band_of(1 - parity, 2 * i), field, tile)
            put(band_of(1 - parity, 2 * i + 1), field, roll(tile, -LATS))
        return carry

    lax.fori_loop(0, NF, one_b, 0)


def per_device(fourier, quad_weights, legendre, slot_wave, vert_proj, vert_recon, vert_rates):
    nlat, total = legendre.shape[1:]
    dense = (NF, ND, 8, 128)
    pair = (HB, NZ, 8, 128)
    vmem, smem = pl.BlockSpec(memory_space=pltpu.VMEM), pl.BlockSpec(memory_space=pltpu.SMEM)
    anywhere = pl.BlockSpec(memory_space=pl.ANY)
    buffers = [dense, dense, pair, pair, pair, pair, dense, dense, dense, dense, pair, dense, pair, pair, dense]
    spectral, last_a, last_b = pl.pallas_call(
        exchange_kernel,
        out_shape=(
            jax.ShapeDtypeStruct((2 * LEV, total), BF16),
            jax.ShapeDtypeStruct(pair, BF16),
            jax.ShapeDtypeStruct(dense, BF16),
        ),
        in_specs=[smem, vmem, vmem, vmem, vmem, anywhere, anywhere],
        out_specs=[vmem, vmem, vmem],
        scratch_shapes=[
            pltpu.VMEM(fourier.shape, BF16),
            pltpu.VMEM((nlat, total), BF16),
            pltpu.VMEM((2 * LEV, nlat), BF16),
            pltpu.VMEM((2 * LEV, total), F32),
        ]
        + [pltpu.VMEM(shape, BF16) for shape in buffers]
        + [pltpu.SemaphoreType.DMA((2,)), pltpu.SemaphoreType.DMA((8,)), pltpu.SemaphoreType.DMA((8,))],
        compiler_params=pltpu.CompilerParams(
            collective_id=0, has_side_effects=True, vmem_limit_bytes=48 * 1024 * 1024),
        name="exchange",
    )(slot_wave, quad_weights.reshape(1, LATS), vert_rates.reshape(LEV, 1), vert_proj, vert_recon, fourier, legendre)
    returned = pl.pallas_call(
        place_kernel,
        out_shape=jax.ShapeDtypeStruct(fourier.shape, BF16),
        in_specs=[smem, vmem, vmem],
        out_specs=vmem,
        name="place",
    )(slot_wave, last_a, last_b)
    return spectral.reshape(1, 2, LEV, total), returned


def solution(mesh):
    placed = (
        P(None, "field", "band"),
        P("band"),
        P(("band", "field"), None, None),
        P(),
        P(),
        P(),
        P(),
    )
    return jax.shard_map(
        per_device,
        mesh=mesh,
        in_specs=placed,
        out_specs=(P(("band", "field"), None, None, None), P(None, "field", "band")),
        check_vma=False,
    )
```

```python
import functools

import jax
import jax.numpy as jnp
from jax import lax
from jax.experimental import pallas as pl
from jax.experimental.pallas import tpu as pltpu
from jax.sharding import PartitionSpec as P

MESH = pl.DeviceIdType.MESH
F32, BF16 = jnp.float32, jnp.bfloat16
LEV = 96
NX, NY, NZ = 4, 8, 12
NB, NF = NX * NY, 2 * NZ
HB = NB // 2
LATS = 56
PAIR = 2 * LATS
TAIL = 128 - PAIR
ND = HB // 2 - 1
Z_ORDER = (6, 5, -5, 4, -4, 3, -3, 2, -2, 1, -1, 0)
Y_ORDER = (4, 3, -3, 2, -2, 1, -1, 0)


def band_of(parity, j):
    return (parity + 2 * (j // NY)) * NY + j % NY


def lanes():
    return lax.broadcasted_iota(jnp.int32, (8, 128), 1)


def roll(v, by):
    return pltpu.roll(v, by % 128, 1)


def dense_to_pair(src, dst, z):
    lane = lanes()
    low = lane < LATS
    halves = []
    for core in range(2):
        f = 2 * z + core
        tiles = [src[f, i].astype(F32) for i in range(ND)]
        last = roll(tiles[0], TAIL)
        for i in range(1, ND):
            last = jnp.where(lane < TAIL * i, last, roll(tiles[i], TAIL + TAIL * i))
        halves.append(tiles + [last])
    for i in range(ND + 1):
        one, two = halves[0][i], halves[1][i]
        dst[2 * i, z] = jnp.where(low, one, roll(two, LATS)).astype(BF16)
        dst[2 * i + 1, z] = jnp.where(low, roll(one, -LATS), two).astype(BF16)


def pair_to_dense(src, z):
    lane = lanes()
    low, body = lane < LATS, lane < PAIR
    first, second = [], []
    for i in range(ND + 1):
        even, odd = src[2 * i, z].astype(F32), src[2 * i + 1, z].astype(F32)
        first.append(jnp.where(low, even, roll(odd, LATS)))
        second.append(jnp.where(low, roll(even, -LATS), odd))
    out = []
    for tiles in (first, second):
        out.append([jnp.where(body, tiles[i], roll(tiles[ND], PAIR - TAIL * i)) for i in range(ND)])
    return out


def parts_of(v):
    high = v.astype(BF16)
    return high, (v - high.astype(F32)).astype(BF16)


def near_exact(left, right):
    high, low = parts_of(right)
    small = jnp.dot(left[0], low, preferred_element_type=F32) + jnp.dot(left[1], high, preferred_element_type=F32)
    return jnp.dot(left[0], high, preferred_element_type=F32) + small


def exchange_kernel(
    waves, quad, rates, proj, recon, fourier, legendre_hbm,
    spectral, last_a, last_b,
    legendre, left, direct,
    sa1, ra1, sa2, ra2, sb1, rb1, sb2, rb2,
    xa, ya, za, xb, yb, zb, vb,
    local_sem, send_sem, recv_sem,
):
    b, f = lax.axis_index("band"), lax.axis_index("field")
    x, y = b // NY, lax.rem(b, NY)
    z, core = f // 2, lax.rem(f, 2)
    parity, mine = lax.rem(x, 2), (x // 2) * NY + y

    barrier = pltpu.get_barrier_semaphore()

    for i in range(1, NF):
        pl.semaphore_signal(barrier, 1, device_id=(b, lax.rem(f + i, NF)), device_id_type=MESH)
    for i in range(1, NB):
        pl.semaphore_signal(barrier, 1, device_id=(lax.rem(b + i, NB), f), device_id_type=MESH)

    table = []
    for part in range(2):
        side = parity if part == 0 else 1 - parity
        tail_at = band_of(side, HB - 2) * LATS
        for i in range(ND):
            row = (part * ND + i) * 128
            at = pl.multiple_of(band_of(side, 2 * i) * LATS, 16)
            table.append(pltpu.make_async_copy(
                legendre_hbm.at[0, pl.ds(at, PAIR)], legendre.at[pl.ds(row, PAIR)], local_sem))
            at = pl.multiple_of(tail_at + TAIL * i, 16)
            table.append(pltpu.make_async_copy(
                legendre_hbm.at[0, pl.ds(at, TAIL)], legendre.at[pl.ds(row + PAIR, TAIL)], local_sem))
    for copy in table:
        copy.start()
    weight = quad[...]

    def picked(band, field):
        wave = waves[band * NF + field]
        return fourier[wave].astype(F32) * weight

    empty = jnp.zeros((8, TAIL), F32)
    body_lanes = lanes() < PAIR

    def joined(first, second):
        return jnp.concatenate([first, second, empty], axis=1)

    def pack_dense(field, carry):
        tiles = [joined(picked(band_of(parity, 2 * i), field), picked(band_of(parity, 2 * i + 1), field))
                 for i in range(ND + 1)]
        for i in range(ND):
            sa1[field, i] = jnp.where(body_lanes, tiles[i], roll(tiles[ND], PAIR - TAIL * i)).astype(BF16)
        return carry

    def pack_pair(j, carry):
        band = (1 - parity + 2 * (j // NY)) * NY + lax.rem(j, NY)
        for k in range(NZ):
            sb1[j, k] = joined(picked(band, 2 * k), picked(band, 2 * k + 1)).astype(BF16)
        return carry

    lax.fori_loop(0, HB, pack_pair, 0, unroll=2)
    lax.fori_loop(0, NF, pack_dense, 0, unroll=3)
    pl.semaphore_wait(barrier, NB + NF - 2)

    def send(src, dst, phase, device):
        pltpu.make_async_remote_copy(
            src_ref=src, dst_ref=dst, send_sem=send_sem.at[phase], recv_sem=recv_sem.at[phase],
            device_id=device, device_id_type=MESH).start()

    def send_field(src, dst, phase):
        for d in Z_ORDER:
            for k in range(2):
                if d == 0 and k == 0:
                    continue
                to = lax.rem(z + d + NZ, NZ) * 2 + lax.rem(core + k, 2)
                send(src.at[to], dst.at[f], phase, (b, to))

    def send_band(src, dst, phase, same):
        steps = (2, 0) if same else (1, 3)
        for dy in Y_ORDER:
            for dx in steps:
                if dx == 0 and dy == 0:
                    continue
                to_x, to_y = lax.rem(x + dx, NX), lax.rem(y + dy + NY, NY)
                to = (to_x // 2) * NY + to_y
                send(src.at[to], dst.at[mine], phase, (to_x * NY + to_y, f))

    def wait_all(ref, phase, count, received):
        some = ref.at[pl.ds(0, count)]
        copy = pltpu.make_async_remote_copy(
            src_ref=some, dst_ref=some, send_sem=send_sem.at[phase], recv_sem=recv_sem.at[phase],
            device_id=(b, f), device_id_type=MESH)
        if received:
            copy.wait_recv()
        else:
            copy.wait_send()

    def over_z(body):
        def step(k, carry):
            body(k)
            return carry

        lax.fori_loop(0, NZ, step, 0, unroll=3)

    def put_dense(src, dst):
        def body(k):
            out = pair_to_dense(src, k)
            for c in range(2):
                for i in range(ND):
                    dst[2 * k + c, i] = out[c][i].astype(BF16)

        over_z(body)

    send_band(sb1, rb1, 1, False)
    send_field(sa1, ra1, 0)
    ra1[f] = sa1[f]

    wait_all(rb1, 1, HB, True)
    put_dense(rb1, sb2)
    send_field(sb2, rb2, 2)
    rb2[f] = sb2[f]

    wait_all(ra1, 0, NF - 1, True)
    over_z(functools.partial(dense_to_pair, ra1, sa2))
    send_band(sa2, ra2, 3, True)
    ra2[mine] = sa2[mine]

    for copy in table:
        copy.wait()
    total = spectral.shape[1]
    step_n = 256
    half_k = ND * 128

    wait_all(ra2, 3, HB - 1, True)

    def left_a(k):
        out = pair_to_dense(ra2, k)
        for i in range(ND):
            both = jnp.concatenate([out[0][i], out[1][i]], axis=0)
            left[pl.ds(pl.multiple_of(16 * k, 16), 16), 128 * i:128 * (i + 1)] = both.astype(BF16)

    over_z(left_a)
    for n in range(0, total, step_n):
        direct[:, n:n + step_n] = jnp.dot(
            left[:, :half_k], legendre[:half_k, n:n + step_n], preferred_element_type=F32)

    wait_all(rb2, 2, NF - 1, True)

    def left_b(k):
        for i in range(ND):
            both = jnp.concatenate([rb2[2 * k, i].astype(F32), rb2[2 * k + 1, i].astype(F32)], axis=0)
            left[pl.ds(pl.multiple_of(16 * k, 16), 16), half_k + 128 * i:half_k + 128 * (i + 1)] = both.astype(BF16)

    over_z(left_b)
    diagonal = lax.broadcasted_iota(jnp.int32, (LEV, LEV), 0) == lax.broadcasted_iota(jnp.int32, (LEV, LEV), 1)
    rate = jnp.sum(jnp.where(diagonal, rates[...], 0.0), axis=1, keepdims=True)
    proj_parts, recon_parts = parts_of(proj[...]), parts_of(recon[...])
    my_wave = waves[b * NF + f]
    for n in range(0, total, step_n):
        part = direct[:, n:n + step_n] + jnp.dot(
            left[:, half_k:], legendre[half_k:, n:n + step_n], preferred_element_type=F32)
        order = (lax.broadcasted_iota(jnp.int32, (LEV, step_n), 1) + n).astype(F32)
        gamma = 1.0 / (1.0 + rate * (order * (order + 1.0) / float(total * total)))
        degree = lax.broadcasted_iota(jnp.int32, (LEV, step_n), 1) + n
        for c in range(2):
            modes = gamma * near_exact(proj_parts, part[LEV * c:LEV * (c + 1)])
            solved = near_exact(recon_parts, modes)
            kept = jnp.where(degree >= my_wave, solved, 0.0)
            spectral[LEV * c:LEV * (c + 1), n:n + step_n] = kept.astype(BF16)

    def back(part, out):
        for i in range(ND):
            row = (part * ND + i) * 128
            made = lax.dot_general(
                spectral[...], legendre[row:row + 128, :], (((1,), (1,)), ((), ())), preferred_element_type=F32)
            out[:, i] = made.reshape(NF, 8, 128).astype(BF16)

    back(1, xb)
    over_z(functools.partial(dense_to_pair, xb, yb))
    send_band(yb, zb, 5, False)
    back(0, xa)
    send_field(xa, ya, 4)
    ya[f] = xa[f]

    wait_all(zb, 5, HB, True)
    put_dense(zb, vb)
    send_field(vb, last_b, 6)
    last_b[f] = vb[f]

    wait_all(ya, 4, NF - 1, True)
    over_z(functools.partial(dense_to_pair, ya, za))
    send_band(za, last_a, 7, True)
    last_a[mine] = za[mine]

    wait_all(last_a, 7, HB - 1, True)
    wait_all(last_b, 6, NF - 1, True)
    for ref, phase, count in (
        (sa1, 0, NF - 1), (sb1, 1, HB), (sb2, 2, NF - 1), (sa2, 3, HB - 1),
        (xa, 4, NF - 1), (yb, 5, HB), (vb, 6, NF - 1), (za, 7, HB - 1),
    ):
        wait_all(ref, phase, count, False)


def place_kernel(waves, from_a, from_b, solved, returned, spectral):
    spectral[...] = solved[...]
    b = lax.axis_index("band")
    parity = lax.rem(b // NY, 2)
    lane = lanes()

    def put(band, field, tile):
        returned[waves[band * NF + field]] = tile[:, :LATS].astype(BF16)

    def one_a(j, carry):
        band = (parity + 2 * (j // NY)) * NY + lax.rem(j, NY)
        for k in range(NZ):
            tile = from_a[j, k].astype(F32)
            put(band, 2 * k, tile)
            put(band, 2 * k + 1, roll(tile, -LATS))
        return carry

    lax.fori_loop(0, HB, one_a, 0, unroll=4)

    def one_b(field, carry):
        tiles = [from_b[field, i].astype(F32) for i in range(ND)]
        last = roll(tiles[0], TAIL)
        for i in range(1, ND):
            last = jnp.where(lane < TAIL * i, last, roll(tiles[i], TAIL + TAIL * i))
        for i, tile in enumerate(tiles + [last]):
            put(band_of(1 - parity, 2 * i), field, tile)
            put(band_of(1 - parity, 2 * i + 1), field, roll(tile, -LATS))
        return carry

    lax.fori_loop(0, NF, one_b, 0, unroll=4)


def per_device(fourier, quad_weights, legendre, slot_wave, vert_proj, vert_recon, vert_rates):
    nlat, total = legendre.shape[1:]
    dense = (NF, ND, 8, 128)
    pair = (HB, NZ, 8, 128)
    vmem, smem = pl.BlockSpec(memory_space=pltpu.VMEM), pl.BlockSpec(memory_space=pltpu.SMEM)
    hbm = pl.BlockSpec(memory_space=pltpu.HBM)
    buffers = [dense, dense, pair, pair, pair, pair, dense, dense, dense, dense, pair, dense, pair, pair, dense]
    spectral, last_a, last_b = pl.pallas_call(
        exchange_kernel,
        out_shape=(
            jax.ShapeDtypeStruct((2 * LEV, total), BF16),
            jax.ShapeDtypeStruct(pair, BF16),
            jax.ShapeDtypeStruct(dense, BF16),
        ),
        in_specs=[smem, vmem, vmem, vmem, vmem, vmem, hbm],
        out_specs=[vmem, vmem, vmem],
        scratch_shapes=[
            pltpu.VMEM((nlat, total), BF16),
            pltpu.VMEM((2 * LEV, nlat), BF16),
            pltpu.VMEM((2 * LEV, total), F32),
        ]
        + [pltpu.VMEM(shape, BF16) for shape in buffers]
        + [pltpu.SemaphoreType.DMA, pltpu.SemaphoreType.DMA((8,)), pltpu.SemaphoreType.DMA((8,))],
        compiler_params=pltpu.CompilerParams(
            collective_id=0, has_side_effects=True, vmem_limit_bytes=52_500_000),
        name="exchange",
    )(slot_wave, quad_weights.reshape(1, LATS), vert_rates.reshape(1, LEV), vert_proj, vert_recon, fourier, legendre)
    returned, spectral = pl.pallas_call(
        place_kernel,
        out_shape=(jax.ShapeDtypeStruct(fourier.shape, BF16), jax.ShapeDtypeStruct(spectral.shape, BF16)),
        in_specs=[smem, vmem, vmem, vmem],
        out_specs=[vmem, vmem],
        compiler_params=pltpu.CompilerParams(vmem_limit_bytes=16 * 1024 * 1024),
        name="place",
    )(slot_wave, last_a, last_b, spectral)
    return spectral.reshape(1, 2, LEV, total), returned


def solution(mesh):
    placed = (
        P(None, "field", "band"),
        P("band"),
        P(("band", "field"), None, None),
        P(),
        P(),
        P(),
        P(),
    )
    return jax.shard_map(
        per_device,
        mesh=mesh,
        in_specs=placed,
        out_specs=(P(("band", "field"), None, None, None), P(None, "field", "band")),
        check_vma=False,
    )
```

```python
import functools

import jax
import jax.numpy as jnp
from jax import lax
from jax.experimental import pallas as pl
from jax.experimental.pallas import tpu as pltpu
from jax.sharding import PartitionSpec as P

MESH = pl.DeviceIdType.MESH
F32, BF16 = jnp.float32, jnp.bfloat16
LEV = 96
NX, NY, NZ = 4, 8, 12
NB, NF = NX * NY, 2 * NZ
HB = NB // 2
LATS = 56
PAIR = 2 * LATS
TAIL = 128 - PAIR
ND = HB // 2 - 1
SKEW = 8 * (ND + 1) + 8
Z_ORDER = (6, 5, -5, 4, -4, 3, -3, 2, -2, 1, -1, 0)
Y_ORDER = (4, 3, -3, 2, -2, 1, -1, 0)


def band_of(parity, j):
    return (parity + 2 * (j // NY)) * NY + j % NY


def lanes():
    return lax.broadcasted_iota(jnp.int32, (8, 128), 1)


def roll(v, by):
    return pltpu.roll(v, by % 128, 1)


def dense_to_pair(src, dst, z):
    lane = lanes()
    low = lane < LATS
    halves = []
    for core in range(2):
        f = 2 * z + core
        tiles = [src[f, i].astype(F32) for i in range(ND)]
        last = roll(tiles[0], TAIL)
        for i in range(1, ND):
            last = jnp.where(lane < TAIL * i, last, roll(tiles[i], TAIL + TAIL * i))
        halves.append(tiles + [last])
    for i in range(ND + 1):
        one, two = halves[0][i], halves[1][i]
        dst[2 * i, z] = jnp.where(low, one, roll(two, LATS)).astype(BF16)
        dst[2 * i + 1, z] = jnp.where(low, roll(one, -LATS), two).astype(BF16)


def pair_to_dense(src, z):
    lane = lanes()
    low, body = lane < LATS, lane < PAIR
    first, second = [], []
    for i in range(ND + 1):
        even, odd = src[2 * i, z].astype(F32), src[2 * i + 1, z].astype(F32)
        first.append(jnp.where(low, even, roll(odd, LATS)))
        second.append(jnp.where(low, roll(even, -LATS), odd))
    out = []
    for tiles in (first, second):
        out.append([jnp.where(body, tiles[i], roll(tiles[ND], PAIR - TAIL * i)) for i in range(ND)])
    return out


def turned(row):
    n = row.shape[1]
    diagonal = lax.broadcasted_iota(jnp.int32, (n, n), 0) == lax.broadcasted_iota(jnp.int32, (n, n), 1)
    return jnp.sum(jnp.where(diagonal, row, 0.0), axis=1, keepdims=True)


def parts_of(v):
    high = v.astype(BF16)
    return high, (v - high.astype(F32)).astype(BF16)


def near_exact(left, right):
    high, low = parts_of(right)
    small = jnp.dot(left[0], low, preferred_element_type=F32) + jnp.dot(left[1], high, preferred_element_type=F32)
    return jnp.dot(left[0], high, preferred_element_type=F32) + small


def exchange_kernel(
    waves_hbm, quad_hbm, rates_hbm, proj_hbm, recon_hbm, fourier_hbm, legendre_hbm,
    spectral, last_a, last_b,
    waves, quad, rates, proj, recon, legendre, left, direct, fourier, weighted, chosen, gathered, tiles_a, tiles_b,
    sa1, ra1, sa2, ra2, sb1, rb1, sb2, rb2,
    xa, ya, za, xb, yb, zb, vb,
    small_sem, local_sem, fetch_sem, send_sem, recv_sem,
):
    b, f = lax.axis_index("band"), lax.axis_index("field")
    x, y = b // NY, lax.rem(b, NY)
    z, core = f // 2, lax.rem(f, 2)
    parity, mine = lax.rem(x, 2), (x // 2) * NY + y

    barrier = pltpu.get_barrier_semaphore()

    small = [
        pltpu.make_async_copy(src, dst, small_sem.at[i])
        for i, (src, dst) in enumerate(
            ((waves_hbm, waves), (quad_hbm, quad), (rates_hbm, rates), (proj_hbm, proj), (recon_hbm, recon)))]
    fetch = pltpu.make_async_copy(fourier_hbm, fourier, fetch_sem)
    for copy in small:
        copy.start()
    fetch.start()

    for i in range(1, NF):
        pl.semaphore_signal(barrier, 1, device_id=(b, lax.rem(f + i, NF)), device_id_type=MESH)
    for i in range(1, NB):
        pl.semaphore_signal(barrier, 1, device_id=(lax.rem(b + i, NB), f), device_id_type=MESH)

    table = []
    for part in range(2):
        side = parity if part == 0 else 1 - parity
        tail_at = band_of(side, HB - 2) * LATS
        for i in range(ND):
            row = (part * ND + i) * 128
            at = pl.multiple_of(band_of(side, 2 * i) * LATS, 16)
            table.append(pltpu.make_async_copy(
                legendre_hbm.at[0, pl.ds(at, PAIR)], legendre.at[pl.ds(row, PAIR)], local_sem))
            at = pl.multiple_of(tail_at + TAIL * i, 16)
            table.append(pltpu.make_async_copy(
                legendre_hbm.at[0, pl.ds(at, TAIL)], legendre.at[pl.ds(row + PAIR, TAIL)], local_sem))
    for copy in table:
        copy.start()
    for copy in small:
        copy.wait()
    total = spectral.shape[1]
    wave_of_lane = lax.broadcasted_iota(jnp.int32, (128, total), 1).astype(F32)
    for t in range(total // 128):
        column = turned(waves[t:t + 1, :].astype(F32))
        chosen[128 * t:128 * (t + 1)] = jnp.where(wave_of_lane == column, 1.0, 0.0).astype(BF16)
    weight = turned(quad[...])
    fetch.wait()
    for r in range(8):
        rows = jnp.concatenate([fourier[r].astype(F32) * weight, jnp.zeros((8, total), F32)], axis=0)
        weighted[64 * r:64 * (r + 1)] = rows.astype(BF16)
    for n in range(2):
        found = lax.dot_general(
            chosen[...], weighted[256 * n:256 * (n + 1)], (((1,), (1,)), ((), ())), preferred_element_type=F32)
        gathered[2 * n] = found[:, :128]
        gathered[2 * n + 1] = found[:, 128:]

    low_lanes, body_lanes = lanes() < LATS, lanes() < PAIR

    def side_by_side(even, odd, r):
        if r % 2 == 0:
            return jnp.where(low_lanes, even, roll(odd, LATS))
        return jnp.where(low_lanes, roll(even, -64), roll(odd, LATS - 64))

    def rows_pair(t, carry):
        for half in range(2):
            start = (1 - parity + 2 * half) * NY * NF + 16 * t
            for r in range(8):
                even = gathered[r // 2, pl.ds(start, 8, stride=2), :]
                odd = gathered[r // 2, pl.ds(start + 1, 8, stride=2), :]
                at = (half * NY * NZ + 8 * t) * 8 + r
                tiles_b[pl.ds(at, 8, stride=8), :] = side_by_side(even, odd, r)
        return carry

    def rows_dense(i, carry):
        band = (parity + 2 * ((2 * i) // NY)) * NY + lax.rem(2 * i, NY)
        for t in range(NF // 8):
            start = pl.multiple_of(band * NF + 8 * t, 8)
            for r in range(8):
                even = gathered[r // 2, pl.ds(start, 8), :]
                odd = gathered[r // 2, pl.ds(pl.multiple_of(start + NF, 8), 8), :]
                at = 8 * t * SKEW + 8 * i + r
                tiles_a[pl.ds(at, 8, stride=SKEW), :] = side_by_side(even, odd, r)
        return carry

    def pack_pair(j, carry):
        for k in range(NZ):
            sb1[j, k] = tiles_b[pl.ds(pl.multiple_of((j * NZ + k) * 8, 8), 8), :].astype(BF16)
        return carry

    def pack_dense(field, carry):
        tiles = [tiles_a[pl.ds(pl.multiple_of(field * SKEW + 8 * i, 8), 8), :] for i in range(ND + 1)]
        for i in range(ND):
            sa1[field, i] = jnp.where(body_lanes, tiles[i], roll(tiles[ND], PAIR - TAIL * i)).astype(BF16)
        return carry

    lax.fori_loop(0, ND + 1, rows_dense, 0, unroll=2)
    lax.fori_loop(0, NF, pack_dense, 0, unroll=3)
    pl.semaphore_wait(barrier, NB + NF - 2)

    def send(src, dst, phase, device):
        pltpu.make_async_remote_copy(
            src_ref=src, dst_ref=dst, send_sem=send_sem.at[phase], recv_sem=recv_sem.at[phase],
            device_id=device, device_id_type=MESH).start()

    def send_field(src, dst, phase):
        for d in Z_ORDER:
            for k in range(2):
                if d == 0 and k == 0:
                    continue
                to = lax.rem(z + d + NZ, NZ) * 2 + lax.rem(core + k, 2)
                send(src.at[to], dst.at[f], phase, (b, to))

    def send_band(src, dst, phase, same):
        steps = (2, 0) if same else (1, 3)
        for dy in Y_ORDER:
            for dx in steps:
                if dx == 0 and dy == 0:
                    continue
                to_x, to_y = lax.rem(x + dx, NX), lax.rem(y + dy + NY, NY)
                to = (to_x // 2) * NY + to_y
                send(src.at[to], dst.at[mine], phase, (to_x * NY + to_y, f))

    def wait_all(ref, phase, count, received):
        some = ref.at[pl.ds(0, count)]
        copy = pltpu.make_async_remote_copy(
            src_ref=some, dst_ref=some, send_sem=send_sem.at[phase], recv_sem=recv_sem.at[phase],
            device_id=(b, f), device_id_type=MESH)
        if received:
            copy.wait_recv()
        else:
            copy.wait_send()

    def over_z(body):
        def step(k, carry):
            body(k)
            return carry

        lax.fori_loop(0, NZ, step, 0, unroll=3)

    def put_dense(src, dst):
        def body(k):
            out = pair_to_dense(src, k)
            for c in range(2):
                for i in range(ND):
                    dst[2 * k + c, i] = out[c][i].astype(BF16)

        over_z(body)

    send_field(sa1, ra1, 0)
    lax.fori_loop(0, NY * NZ // 8, rows_pair, 0, unroll=2)
    lax.fori_loop(0, HB, pack_pair, 0, unroll=2)
    send_band(sb1, rb1, 1, False)
    ra1[f] = sa1[f]

    wait_all(rb1, 1, HB, True)
    put_dense(rb1, sb2)
    send_field(sb2, rb2, 2)
    rb2[f] = sb2[f]

    wait_all(ra1, 0, NF - 1, True)
    over_z(functools.partial(dense_to_pair, ra1, sa2))
    send_band(sa2, ra2, 3, True)
    ra2[mine] = sa2[mine]

    for copy in table:
        copy.wait()
    step_n = 256
    half_k = ND * 128

    wait_all(ra2, 3, HB - 1, True)

    def left_a(k):
        out = pair_to_dense(ra2, k)
        for i in range(ND):
            both = jnp.concatenate([out[0][i], out[1][i]], axis=0)
            left[pl.ds(pl.multiple_of(16 * k, 16), 16), 128 * i:128 * (i + 1)] = both.astype(BF16)

    over_z(left_a)
    for n in range(0, total, step_n):
        direct[:, n:n + step_n] = jnp.dot(
            left[:, :half_k], legendre[:half_k, n:n + step_n], preferred_element_type=F32)

    wait_all(rb2, 2, NF - 1, True)

    def left_b(k):
        for i in range(ND):
            both = jnp.concatenate([rb2[2 * k, i].astype(F32), rb2[2 * k + 1, i].astype(F32)], axis=0)
            left[pl.ds(pl.multiple_of(16 * k, 16), 16), half_k + 128 * i:half_k + 128 * (i + 1)] = both.astype(BF16)

    over_z(left_b)
    rate = turned(rates[...])
    proj_parts, recon_parts = parts_of(proj[...]), parts_of(recon[...])
    place_of = lax.broadcasted_iota(jnp.int32, waves.shape, 0) * 128 + lax.broadcasted_iota(jnp.int32, waves.shape, 1)
    mine_only = jnp.where(place_of == b * NF + f, waves[...].astype(F32), 0.0)
    my_wave = jnp.sum(jnp.sum(mine_only, axis=1, keepdims=True), axis=0, keepdims=True)
    for n in range(0, total, step_n):
        part = direct[:, n:n + step_n] + jnp.dot(
            left[:, half_k:], legendre[half_k:, n:n + step_n], preferred_element_type=F32)
        order = (lax.broadcasted_iota(jnp.int32, (LEV, step_n), 1) + n).astype(F32)
        gamma = 1.0 / (1.0 + rate * (order * (order + 1.0) / float(total * total)))
        for c in range(2):
            modes = gamma * near_exact(proj_parts, part[LEV * c:LEV * (c + 1)])
            solved = near_exact(recon_parts, modes)
            kept = jnp.where(order >= my_wave, solved, 0.0)
            spectral[LEV * c:LEV * (c + 1), n:n + step_n] = kept.astype(BF16)

    def back(part, out):
        for i in range(ND):
            row = (part * ND + i) * 128
            made = lax.dot_general(
                spectral[...], legendre[row:row + 128, :], (((1,), (1,)), ((), ())), preferred_element_type=F32)
            out[:, i] = made.reshape(NF, 8, 128).astype(BF16)

    back(1, xb)
    over_z(functools.partial(dense_to_pair, xb, yb))
    send_band(yb, zb, 5, False)
    back(0, xa)
    send_field(xa, ya, 4)
    ya[f] = xa[f]

    wait_all(zb, 5, HB, True)
    put_dense(zb, vb)
    send_field(vb, last_b, 6)
    last_b[f] = vb[f]

    wait_all(ya, 4, NF - 1, True)
    over_z(functools.partial(dense_to_pair, ya, za))
    send_band(za, last_a, 7, True)
    last_a[mine] = za[mine]

    wait_all(last_a, 7, HB - 1, True)
    wait_all(last_b, 6, NF - 1, True)
    for ref, phase, count in (
        (sa1, 0, NF - 1), (sb1, 1, HB), (sb2, 2, NF - 1), (sa2, 3, HB - 1),
        (xa, 4, NF - 1), (yb, 5, HB), (vb, 6, NF - 1), (za, 7, HB - 1),
    ):
        wait_all(ref, phase, count, False)


def place_kernel(waves, from_a, from_b, solved, returned, spectral):
    spectral[...] = solved[...]
    b = lax.axis_index("band")
    parity = lax.rem(b // NY, 2)
    lane = lanes()

    def put(band, field, tile):
        returned[waves[band * NF + field]] = tile[:, :LATS].astype(BF16)

    def one_a(j, carry):
        band = (parity + 2 * (j // NY)) * NY + lax.rem(j, NY)
        for k in range(NZ):
            tile = from_a[j, k].astype(F32)
            put(band, 2 * k, tile)
            put(band, 2 * k + 1, roll(tile, -LATS))
        return carry

    lax.fori_loop(0, HB, one_a, 0, unroll=4)

    def one_b(field, carry):
        tiles = [from_b[field, i].astype(F32) for i in range(ND)]
        last = roll(tiles[0], TAIL)
        for i in range(1, ND):
            last = jnp.where(lane < TAIL * i, last, roll(tiles[i], TAIL + TAIL * i))
        for i, tile in enumerate(tiles + [last]):
            put(band_of(1 - parity, 2 * i), field, tile)
            put(band_of(1 - parity, 2 * i + 1), field, roll(tile, -LATS))
        return carry

    lax.fori_loop(0, NF, one_b, 0, unroll=4)


def per_device(fourier, quad_weights, legendre, slot_wave, vert_proj, vert_recon, vert_rates):
    nlat, total = legendre.shape[1:]
    dense = (NF, ND, 8, 128)
    pair = (HB, NZ, 8, 128)
    vmem, smem = pl.BlockSpec(memory_space=pltpu.VMEM), pl.BlockSpec(memory_space=pltpu.SMEM)
    hbm = pl.BlockSpec(memory_space=pltpu.HBM)
    buffers = [dense, dense, pair, pair, pair, pair, dense, dense, dense, dense, pair, dense, pair, pair, dense]
    spectral, last_a, last_b = pl.pallas_call(
        exchange_kernel,
        out_shape=(
            jax.ShapeDtypeStruct((2 * LEV, total), BF16),
            jax.ShapeDtypeStruct(pair, BF16),
            jax.ShapeDtypeStruct(dense, BF16),
        ),
        in_specs=[hbm] * 7,
        out_specs=[vmem, vmem, vmem],
        scratch_shapes=[
            pltpu.VMEM((total // 128, 128), jnp.int32),
            pltpu.VMEM((1, LATS), F32),
            pltpu.VMEM((1, LEV), F32),
            pltpu.VMEM((LEV, LEV), F32),
            pltpu.VMEM((LEV, LEV), F32),
            pltpu.VMEM((nlat, total), BF16),
            pltpu.VMEM((2 * LEV, nlat), BF16),
            pltpu.VMEM((2 * LEV, total), F32),
            pltpu.VMEM((8, LATS, total), BF16),
            pltpu.VMEM((512, total), BF16),
            pltpu.VMEM((total, total), BF16),
            pltpu.VMEM((4, total, 128), F32),
            pltpu.VMEM((NF * SKEW, 128), F32),
            pltpu.VMEM((HB * NZ * 8, 128), F32),
        ]
        + [pltpu.VMEM(shape, BF16) for shape in buffers]
        + [pltpu.SemaphoreType.DMA((5,)), pltpu.SemaphoreType.DMA, pltpu.SemaphoreType.DMA, pltpu.SemaphoreType.DMA((8,)), pltpu.SemaphoreType.DMA((8,))],
        compiler_params=pltpu.CompilerParams(
            collective_id=0, has_side_effects=True, vmem_limit_bytes=55_000_000),
        name="exchange",
    )(*[pltpu.with_memory_space_constraint(v, pltpu.HBM) for v in (
        slot_wave.reshape(total // 128, 128), quad_weights.reshape(1, LATS), vert_rates.reshape(1, LEV),
        vert_proj, vert_recon, jnp.transpose(fourier, (1, 2, 0)), legendre)])
    returned, spectral = pl.pallas_call(
        place_kernel,
        out_shape=(jax.ShapeDtypeStruct(fourier.shape, BF16), jax.ShapeDtypeStruct(spectral.shape, BF16)),
        in_specs=[smem, vmem, vmem, vmem],
        out_specs=[vmem, vmem],
        compiler_params=pltpu.CompilerParams(vmem_limit_bytes=16 * 1024 * 1024),
        name="place",
    )(slot_wave, last_a, last_b, spectral)
    return spectral.reshape(1, 2, LEV, total), returned


def solution(mesh):
    placed = (
        P(None, "field", "band"),
        P("band"),
        P(("band", "field"), None, None),
        P(),
        P(),
        P(),
        P(),
    )
    return jax.shard_map(
        per_device,
        mesh=mesh,
        in_specs=placed,
        out_specs=(P(("band", "field"), None, None, None), P(None, "field", "band")),
        check_vma=False,
    )
```

```python
import functools

import jax
import jax.numpy as jnp
from jax import lax
from jax.experimental import pallas as pl
from jax.experimental.pallas import tpu as pltpu
from jax.sharding import PartitionSpec as P

MESH = pl.DeviceIdType.MESH
F32, BF16 = jnp.float32, jnp.bfloat16
LEV = 96
NX, NY, NZ = 4, 8, 12
NB, NF = NX * NY, 2 * NZ
HB = NB // 2
LATS = 56
PAIR = 2 * LATS
TAIL = 128 - PAIR
ND = HB // 2 - 1
SKEW = 8 * (ND + 1) + 8
FAR = 4
CHUNKS = ((0, 5), (5, 7))
Z_ORDERS = ((6, 5, -5, 4, -4), (3, -3, 2, -2, 1, -1, 0))
Y_ORDER = (4, 3, -3, 2, -2, 1, -1, 0)


def band_of(parity, j):
    return (parity + 2 * (j // NY)) * NY + j % NY


def lanes():
    return lax.broadcasted_iota(jnp.int32, (8, 128), 1)


def roll(v, by):
    return pltpu.roll(v, by % 128, 1)


def chip_of(z, t):
    return lax.rem(z + FAR + t, NZ)


def dense_to_pair(src, dst, z, t):
    lane = lanes()
    low = lane < LATS
    halves = []
    for core in range(2):
        f = 2 * chip_of(z, t) + core
        tiles = [src[f, i].astype(F32) for i in range(ND)]
        last = roll(tiles[0], TAIL)
        for i in range(1, ND):
            last = jnp.where(lane < TAIL * i, last, roll(tiles[i], TAIL + TAIL * i))
        halves.append(tiles + [last])
    for i in range(ND + 1):
        one, two = halves[0][i], halves[1][i]
        dst[2 * i, t] = jnp.where(low, one, roll(two, LATS)).astype(BF16)
        dst[2 * i + 1, t] = jnp.where(low, roll(one, -LATS), two).astype(BF16)


def pair_to_dense(src, t):
    lane = lanes()
    low, body = lane < LATS, lane < PAIR
    first, second = [], []
    for i in range(ND + 1):
        even, odd = src[2 * i, t].astype(F32), src[2 * i + 1, t].astype(F32)
        first.append(jnp.where(low, even, roll(odd, LATS)))
        second.append(jnp.where(low, roll(even, -LATS), odd))
    out = []
    for tiles in (first, second):
        out.append([jnp.where(body, tiles[i], roll(tiles[ND], PAIR - TAIL * i)) for i in range(ND)])
    return out


def turned(row):
    n = row.shape[1]
    diagonal = lax.broadcasted_iota(jnp.int32, (n, n), 0) == lax.broadcasted_iota(jnp.int32, (n, n), 1)
    return jnp.sum(jnp.where(diagonal, row, 0.0), axis=1, keepdims=True)


def parts_of(v):
    high = v.astype(BF16)
    return high, (v - high.astype(F32)).astype(BF16)


def near_exact(left, right):
    n = left.shape[0] // 2
    high, low = parts_of(right)
    both = jnp.dot(left, high, preferred_element_type=F32)
    return both[:n] + (both[n:] + jnp.dot(left[:n], low, preferred_element_type=F32))


def exchange_kernel(
    waves_hbm, quad_hbm, rates_hbm, proj_hbm, recon_hbm, fourier_hbm, legendre_hbm,
    spectral, last_a, last_b,
    waves, quad, rates, proj, recon, legendre, left, direct, fourier, weighted, chosen, gathered, tiles_a, tiles_b,
    sa1, ra1, sa2, ra2, sb1, rb1, sb2, rb2,
    xa, ya, za, xb, yb, zb, vb,
    small_sem, local_sem, fetch_sem, send_sem, recv_sem,
):
    b, f = lax.axis_index("band"), lax.axis_index("field")
    x, y = b // NY, lax.rem(b, NY)
    z, core = f // 2, lax.rem(f, 2)
    parity, mine = lax.rem(x, 2), (x // 2) * NY + y

    barrier = pltpu.get_barrier_semaphore()

    small = [
        pltpu.make_async_copy(src, dst, small_sem.at[i])
        for i, (src, dst) in enumerate(
            ((waves_hbm, waves), (quad_hbm, quad), (rates_hbm, rates), (proj_hbm, proj), (recon_hbm, recon)))]
    fetch = pltpu.make_async_copy(fourier_hbm, fourier, fetch_sem)
    for copy in small:
        copy.start()
    fetch.start()

    greeted = [(abs(d), "field", d, k) for order in Z_ORDERS for d in order for k in range(2) if (d, k) != (0, 0)]
    greeted += [
        (min(dx, NX - dx) + abs(dy), "band", dx, dy) for dy in Y_ORDER for dx in range(NX) if (dx, dy) != (0, 0)]
    for _, axis, one, two in sorted(greeted, key=lambda item: -item[0]):
        if axis == "field":
            to = (b, lax.rem(z + one + NZ, NZ) * 2 + lax.rem(core + two, 2))
        else:
            to = (lax.rem(x + one, NX) * NY + lax.rem(y + two + NY, NY), f)
        pl.semaphore_signal(barrier, 1, device_id=to, device_id_type=MESH)

    table = []
    for part in range(2):
        side = parity if part == 0 else 1 - parity
        tail_at = band_of(side, HB - 2) * LATS
        for i in range(ND):
            row = (part * ND + i) * 128
            at = pl.multiple_of(band_of(side, 2 * i) * LATS, 16)
            table.append(pltpu.make_async_copy(
                legendre_hbm.at[0, pl.ds(at, PAIR)], legendre.at[pl.ds(row, PAIR)], local_sem))
            at = pl.multiple_of(tail_at + TAIL * i, 16)
            table.append(pltpu.make_async_copy(
                legendre_hbm.at[0, pl.ds(at, TAIL)], legendre.at[pl.ds(row + PAIR, TAIL)], local_sem))
    for copy in table:
        copy.start()
    for copy in small:
        copy.wait()
    total = spectral.shape[1]
    wave_of_lane = lax.broadcasted_iota(jnp.int32, (128, total), 1).astype(F32)
    for t in range(total // 128):
        column = turned(waves[t:t + 1, :].astype(F32))
        chosen[128 * t:128 * (t + 1)] = jnp.where(wave_of_lane == column, 1.0, 0.0).astype(BF16)
    weight = turned(quad[...])
    fetch.wait()
    for r in range(8):
        rows = jnp.concatenate([fourier[r].astype(F32) * weight, jnp.zeros((8, total), F32)], axis=0)
        weighted[64 * r:64 * (r + 1)] = rows.astype(BF16)
    for n in range(2):
        found = lax.dot_general(
            chosen[...], weighted[256 * n:256 * (n + 1)], (((1,), (1,)), ((), ())), preferred_element_type=F32)
        gathered[2 * n] = found[:, :128]
        gathered[2 * n + 1] = found[:, 128:]

    low_lanes, body_lanes = lanes() < LATS, lanes() < PAIR

    def side_by_side(even, odd, r):
        if r % 2 == 0:
            return jnp.where(low_lanes, even, roll(odd, LATS))
        return jnp.where(low_lanes, roll(even, -64), roll(odd, LATS - 64))

    def rows_pair(t, carry):
        for half in range(2):
            start = (1 - parity + 2 * half) * NY * NF + 16 * t
            for r in range(8):
                even = gathered[r // 2, pl.ds(start, 8, stride=2), :]
                odd = gathered[r // 2, pl.ds(start + 1, 8, stride=2), :]
                at = (half * NY * NZ + 8 * t) * 8 + r
                tiles_b[pl.ds(at, 8, stride=8), :] = side_by_side(even, odd, r)
        return carry

    def rows_dense(i, carry):
        band = (parity + 2 * ((2 * i) // NY)) * NY + lax.rem(2 * i, NY)
        for t in range(NF // 8):
            start = pl.multiple_of(band * NF + 8 * t, 8)
            for r in range(8):
                even = gathered[r // 2, pl.ds(start, 8), :]
                odd = gathered[r // 2, pl.ds(pl.multiple_of(start + NF, 8), 8), :]
                at = 8 * t * SKEW + 8 * i + r
                tiles_a[pl.ds(at, 8, stride=SKEW), :] = side_by_side(even, odd, r)
        return carry

    def pack_pair(j, carry):
        for k in range(NZ):
            sb1[j, k] = tiles_b[pl.ds(pl.multiple_of((j * NZ + chip_of(z, k)) * 8, 8), 8), :].astype(BF16)
        return carry

    def pack_dense(field, carry):
        tiles = [tiles_a[pl.ds(pl.multiple_of(field * SKEW + 8 * i, 8), 8), :] for i in range(ND + 1)]
        for i in range(ND):
            sa1[field, i] = jnp.where(body_lanes, tiles[i], roll(tiles[ND], PAIR - TAIL * i)).astype(BF16)
        return carry

    lax.fori_loop(0, ND + 1, rows_dense, 0, unroll=2)
    lax.fori_loop(0, NF, pack_dense, 0, unroll=3)
    pl.semaphore_wait(barrier, NB + NF - 2)

    def send(src, dst, phase, device):
        pltpu.make_async_remote_copy(
            src_ref=src, dst_ref=dst, send_sem=send_sem.at[phase], recv_sem=recv_sem.at[phase],
            device_id=device, device_id_type=MESH).start()

    def send_field(src, dst, phase, chunk):
        for d in Z_ORDERS[chunk]:
            for k in range(2):
                if d == 0 and k == 0:
                    continue
                to = lax.rem(z + d + NZ, NZ) * 2 + lax.rem(core + k, 2)
                send(src.at[to], dst.at[f], 2 * phase + chunk, (b, to))
        if chunk == 1:
            dst[f] = src[f]

    def send_band(src, dst, phase, chunk, same):
        part = pl.ds(*CHUNKS[chunk])
        for dy in Y_ORDER:
            for dx in (2, 0) if same else (1, 3):
                if dx == 0 and dy == 0:
                    continue
                to_x, to_y = lax.rem(x + dx, NX), lax.rem(y + dy + NY, NY)
                to = (to_x // 2) * NY + to_y
                send(src.at[to, part], dst.at[mine, part], 2 * phase + chunk, (to_x * NY + to_y, f))
        if same:
            dst[mine, part] = src[mine, part]

    def wait_some(some, phase, received):
        copy = pltpu.make_async_remote_copy(
            src_ref=some, dst_ref=some, send_sem=send_sem.at[phase], recv_sem=recv_sem.at[phase],
            device_id=(b, f), device_id_type=MESH)
        if received:
            copy.wait_recv()
        else:
            copy.wait_send()

    def wait_field(ref, phase, chunk, received=True):
        wait_some(ref.at[pl.ds(0, (10, 13)[chunk])], 2 * phase + chunk, received)

    def wait_band(ref, phase, chunk, same, received=True):
        wait_some(ref.at[pl.ds(0, HB - 1 if same else HB), pl.ds(*CHUNKS[chunk])], 2 * phase + chunk, received)

    def over_chunk(chunk, body):
        first, count = CHUNKS[chunk]

        def step(k, carry):
            body(first + k)
            return carry

        lax.fori_loop(0, count, step, 0, unroll=count)

    def put_dense(src, dst, chunk):
        def body(t):
            out = pair_to_dense(src, t)
            for c in range(2):
                for i in range(ND):
                    dst[2 * chip_of(z, t) + c, i] = out[c][i].astype(BF16)

        over_chunk(chunk, body)

    def put_pair(src, dst, chunk):
        over_chunk(chunk, functools.partial(dense_to_pair, src, dst, z))

    for chunk in range(2):
        send_field(sa1, ra1, 0, chunk)
    lax.fori_loop(0, NY * NZ // 8, rows_pair, 0, unroll=2)
    lax.fori_loop(0, HB, pack_pair, 0, unroll=2)
    for chunk in range(2):
        send_band(sb1, rb1, 1, chunk, False)

    def second_phase(in_b, out_b, end_b, in_a, out_a, end_a, phase):
        for chunk in range(2):
            wait_band(in_b, phase + 1, chunk, False)
            put_dense(in_b, out_b, chunk)
            send_field(out_b, end_b, phase + 2, chunk)
            wait_field(in_a, phase, chunk)
            put_pair(in_a, out_a, chunk)
            send_band(out_a, end_a, phase + 3, chunk, True)

    second_phase(rb1, sb2, rb2, ra1, sa2, ra2, 0)
    for copy in table:
        copy.wait()
    step_n = 256
    half_k = ND * 128

    def left_a(t):
        out = pair_to_dense(ra2, t)
        row = pl.multiple_of(16 * chip_of(z, t), 16)
        for i in range(ND):
            both = jnp.concatenate([out[0][i], out[1][i]], axis=0)
            left[pl.ds(row, 16), 128 * i:128 * (i + 1)] = both.astype(BF16)

    for chunk in range(2):
        wait_band(ra2, 3, chunk, True)
        over_chunk(chunk, left_a)
    for n in range(0, total, step_n):
        direct[:, n:n + step_n] = jnp.dot(
            left[:, :half_k], legendre[:half_k, n:n + step_n], preferred_element_type=F32)

    for chunk in range(2):
        wait_field(rb2, 2, chunk)

    def left_b(k, carry):
        for i in range(ND):
            both = jnp.concatenate([rb2[2 * k, i].astype(F32), rb2[2 * k + 1, i].astype(F32)], axis=0)
            left[pl.ds(pl.multiple_of(16 * k, 16), 16), half_k + 128 * i:half_k + 128 * (i + 1)] = both.astype(BF16)
        return carry

    lax.fori_loop(0, NZ, left_b, 0, unroll=3)
    rate = turned(rates[...])
    proj_parts = jnp.concatenate(parts_of(proj[...]), axis=0)
    recon_parts = jnp.concatenate(parts_of(recon[...]), axis=0)
    place_of = lax.broadcasted_iota(jnp.int32, waves.shape, 0) * 128 + lax.broadcasted_iota(jnp.int32, waves.shape, 1)
    mine_only = jnp.where(place_of == b * NF + f, waves[...].astype(F32), 0.0)
    my_wave = jnp.sum(jnp.sum(mine_only, axis=1, keepdims=True), axis=0, keepdims=True)
    for n in range(0, total, step_n):
        part = direct[:, n:n + step_n] + jnp.dot(
            left[:, half_k:], legendre[half_k:, n:n + step_n], preferred_element_type=F32)
        order = (lax.broadcasted_iota(jnp.int32, (LEV, step_n), 1) + n).astype(F32)
        gamma = 1.0 / (1.0 + rate * (order * (order + 1.0) / float(total * total)))
        for c in range(2):
            modes = gamma * near_exact(proj_parts, part[LEV * c:LEV * (c + 1)])
            solved = near_exact(recon_parts, modes)
            kept = jnp.where(order >= my_wave, solved, 0.0)
            spectral[LEV * c:LEV * (c + 1), n:n + step_n] = kept.astype(BF16)

    def back(part, out):
        for i in range(ND):
            row = (part * ND + i) * 128
            made = lax.dot_general(
                spectral[...], legendre[row:row + 128, :], (((1,), (1,)), ((), ())), preferred_element_type=F32)
            out[:, i] = made.reshape(NF, 8, 128).astype(BF16)

    back(0, xa)
    for chunk in range(2):
        send_field(xa, ya, 4, chunk)
    back(1, xb)
    for chunk in range(2):
        put_pair(xb, yb, chunk)
        send_band(yb, zb, 5, chunk, False)

    second_phase(zb, vb, last_b, ya, za, last_a, 4)
    for chunk in range(2):
        wait_band(last_a, 7, chunk, True)
    for chunk in range(2):
        wait_field(last_b, 6, chunk)
    for chunk in range(2):
        for ref, phase in ((sa1, 0), (sb2, 2), (xa, 4), (vb, 6)):
            wait_field(ref, phase, chunk, received=False)
        for ref, phase, same in ((sb1, 1, False), (sa2, 3, True), (yb, 5, False), (za, 7, True)):
            wait_band(ref, phase, chunk, same, received=False)


def place_kernel(waves, from_a, from_b, solved, returned, spectral):
    spectral[...] = solved[...]
    b = lax.axis_index("band")
    parity = lax.rem(b // NY, 2)
    z = lax.axis_index("field") // 2
    lane = lanes()

    def put(band, field, tile):
        returned[waves[band * NF + field]] = tile[:, :LATS].astype(BF16)

    def one_a(j, carry):
        band = (parity + 2 * (j // NY)) * NY + lax.rem(j, NY)
        for k in range(NZ):
            tile = from_a[j, k].astype(F32)
            put(band, 2 * chip_of(z, k), tile)
            put(band, 2 * chip_of(z, k) + 1, roll(tile, -LATS))
        return carry

    lax.fori_loop(0, HB, one_a, 0, unroll=4)

    def one_b(field, carry):
        tiles = [from_b[field, i].astype(F32) for i in range(ND)]
        last = roll(tiles[0], TAIL)
        for i in range(1, ND):
            last = jnp.where(lane < TAIL * i, last, roll(tiles[i], TAIL + TAIL * i))
        for i, tile in enumerate(tiles + [last]):
            put(band_of(1 - parity, 2 * i), field, tile)
            put(band_of(1 - parity, 2 * i + 1), field, roll(tile, -LATS))
        return carry

    lax.fori_loop(0, NF, one_b, 0, unroll=4)


def per_device(fourier, quad_weights, legendre, slot_wave, vert_proj, vert_recon, vert_rates):
    nlat, total = legendre.shape[1:]
    dense = (NF, ND, 8, 128)
    pair = (HB, NZ, 8, 128)
    vmem, smem = pl.BlockSpec(memory_space=pltpu.VMEM), pl.BlockSpec(memory_space=pltpu.SMEM)
    hbm = pl.BlockSpec(memory_space=pltpu.HBM)
    buffers = [dense, dense, pair, pair, pair, pair, dense, dense, dense, dense, pair, dense, pair, pair, dense]
    spectral, last_a, last_b = pl.pallas_call(
        exchange_kernel,
        out_shape=(
            jax.ShapeDtypeStruct((2 * LEV, total), BF16),
            jax.ShapeDtypeStruct(pair, BF16),
            jax.ShapeDtypeStruct(dense, BF16),
        ),
        in_specs=[hbm] * 7,
        out_specs=[vmem, vmem, vmem],
        scratch_shapes=[
            pltpu.VMEM((total // 128, 128), jnp.int32),
            pltpu.VMEM((1, LATS), F32),
            pltpu.VMEM((1, LEV), F32),
            pltpu.VMEM((LEV, LEV), F32),
            pltpu.VMEM((LEV, LEV), F32),
            pltpu.VMEM((nlat, total), BF16),
            pltpu.VMEM((2 * LEV, nlat), BF16),
            pltpu.VMEM((2 * LEV, total), F32),
            pltpu.VMEM((8, LATS, total), BF16),
            pltpu.VMEM((512, total), BF16),
            pltpu.VMEM((total, total), BF16),
            pltpu.VMEM((4, total, 128), F32),
            pltpu.VMEM((NF * SKEW, 128), F32),
            pltpu.VMEM((HB * NZ * 8, 128), F32),
        ]
        + [pltpu.VMEM(shape, BF16) for shape in buffers]
        + [pltpu.SemaphoreType.DMA((5,)), pltpu.SemaphoreType.DMA, pltpu.SemaphoreType.DMA, pltpu.SemaphoreType.DMA((16,)), pltpu.SemaphoreType.DMA((16,))],
        compiler_params=pltpu.CompilerParams(
            collective_id=0, has_side_effects=True, vmem_limit_bytes=55_000_000),
        name="exchange",
    )(*[pltpu.with_memory_space_constraint(v, pltpu.HBM) for v in (
        slot_wave.reshape(total // 128, 128), quad_weights.reshape(1, LATS), vert_rates.reshape(1, LEV),
        vert_proj, vert_recon, jnp.transpose(fourier, (1, 2, 0)), legendre)])
    returned, spectral = pl.pallas_call(
        place_kernel,
        out_shape=(jax.ShapeDtypeStruct(fourier.shape, BF16), jax.ShapeDtypeStruct(spectral.shape, BF16)),
        in_specs=[smem, vmem, vmem, vmem],
        out_specs=[vmem, vmem],
        compiler_params=pltpu.CompilerParams(vmem_limit_bytes=16 * 1024 * 1024),
        name="place",
    )(slot_wave, last_a, last_b, spectral)
    return spectral.reshape(1, 2, LEV, total), returned


def solution(mesh):
    placed = (
        P(None, "field", "band"),
        P("band"),
        P(("band", "field"), None, None),
        P(),
        P(),
        P(),
        P(),
    )
    return jax.shard_map(
        per_device,
        mesh=mesh,
        in_specs=placed,
        out_specs=(P(("band", "field"), None, None, None), P(None, "field", "band")),
        check_vma=False,
    )
```

```python
import functools

import jax
import jax.numpy as jnp
from jax import lax
from jax.experimental import pallas as pl
from jax.experimental.pallas import tpu as pltpu
from jax.sharding import PartitionSpec as P

MESH = pl.DeviceIdType.MESH
F32, BF16 = jnp.float32, jnp.bfloat16
LEV = 96
NX, NY, NZ = 4, 8, 12
NB, NF = NX * NY, 2 * NZ
HB = NB // 2
LATS = 56
PAIR = 2 * LATS
TAIL = 128 - PAIR
ND = HB // 2 - 1
SKEW = 8 * (ND + 1) + 8
FAR = 4
CHUNKS = ((0, 5), (5, 7))
Z_ORDERS = ((6, 5, -5, 4, -4), (3, -3, 2, -2, 1, -1, 0))
Y_ORDER = (4, 3, -3, 2, -2, 1, -1, 0)


def band_of(parity, j):
    return (parity + 2 * (j // NY)) * NY + j % NY


def lanes():
    return lax.broadcasted_iota(jnp.int32, (8, 128), 1)


def roll(v, by):
    return pltpu.roll(v, by % 128, 1)


def chip_of(z, t):
    return lax.rem(z + FAR + t, NZ)


def dense_to_pair(src, dst, z, t):
    lane = lanes()
    low = lane < LATS
    halves = []
    for core in range(2):
        f = 2 * chip_of(z, t) + core
        tiles = [src[f, i].astype(F32) for i in range(ND)]
        last = roll(tiles[0], TAIL)
        for i in range(1, ND):
            last = jnp.where(lane < TAIL * i, last, roll(tiles[i], TAIL + TAIL * i))
        halves.append(tiles + [last])
    for i in range(ND + 1):
        one, two = halves[0][i], halves[1][i]
        dst[2 * i, t] = jnp.where(low, one, roll(two, LATS)).astype(BF16)
        dst[2 * i + 1, t] = jnp.where(low, roll(one, -LATS), two).astype(BF16)


def pair_to_dense(src, t):
    lane = lanes()
    low, body = lane < LATS, lane < PAIR
    first, second = [], []
    for i in range(ND + 1):
        even, odd = src[2 * i, t].astype(F32), src[2 * i + 1, t].astype(F32)
        first.append(jnp.where(low, even, roll(odd, LATS)))
        second.append(jnp.where(low, roll(even, -LATS), odd))
    out = []
    for tiles in (first, second):
        out.append([jnp.where(body, tiles[i], roll(tiles[ND], PAIR - TAIL * i)) for i in range(ND)])
    return out


def turned(row):
    n = row.shape[1]
    diagonal = lax.broadcasted_iota(jnp.int32, (n, n), 0) == lax.broadcasted_iota(jnp.int32, (n, n), 1)
    return jnp.sum(jnp.where(diagonal, row, 0.0), axis=1, keepdims=True)


def parts_of(v):
    high = v.astype(BF16)
    return high, (v - high.astype(F32)).astype(BF16)


def near_exact(left, right):
    n = left.shape[0] // 2
    high, low = parts_of(right)
    both = jnp.dot(left, high, preferred_element_type=F32)
    return both[:n] + (both[n:] + jnp.dot(left[:n], low, preferred_element_type=F32))


def exchange_kernel(
    waves_hbm, quad_hbm, rates_hbm, proj_hbm, recon_hbm, fourier_hbm, legendre_hbm,
    spectral, last_a, last_b,
    waves, quad, rates, proj, recon, gamma, keep, proj_parts, recon_parts, modes,
    legendre, left, direct, fourier, weighted, chosen, gathered, tiles_a, tiles_b,
    sa1, ra1, sa2, ra2, sb1, rb1, sb2, rb2,
    xa, ya, za, xb, yb, zb, vb,
    small_sem, local_sem, fetch_sem, send_sem, recv_sem,
):
    b, f = lax.axis_index("band"), lax.axis_index("field")
    x, y = b // NY, lax.rem(b, NY)
    z, core = f // 2, lax.rem(f, 2)
    parity, mine = lax.rem(x, 2), (x // 2) * NY + y

    barrier = pltpu.get_barrier_semaphore()

    small = [
        pltpu.make_async_copy(src, dst, small_sem.at[i])
        for i, (src, dst) in enumerate(
            ((waves_hbm, waves), (quad_hbm, quad), (rates_hbm, rates), (proj_hbm, proj), (recon_hbm, recon)))]
    fetch = pltpu.make_async_copy(fourier_hbm, fourier, fetch_sem)
    for copy in small:
        copy.start()
    fetch.start()

    greeted = [(abs(d), "field", d, k) for order in Z_ORDERS for d in order for k in range(2) if (d, k) != (0, 0)]
    greeted += [
        (min(dx, NX - dx) + abs(dy), "band", dx, dy) for dy in Y_ORDER for dx in range(NX) if (dx, dy) != (0, 0)]
    for _, axis, one, two in sorted(greeted, key=lambda item: -item[0]):
        if axis == "field":
            to = (b, lax.rem(z + one + NZ, NZ) * 2 + lax.rem(core + two, 2))
        else:
            to = (lax.rem(x + one, NX) * NY + lax.rem(y + two + NY, NY), f)
        pl.semaphore_signal(barrier, 1, device_id=to, device_id_type=MESH)

    table = []
    for part in range(2):
        side = parity if part == 0 else 1 - parity
        tail_at = band_of(side, HB - 2) * LATS
        for i in range(ND):
            row = (part * ND + i) * 128
            at = pl.multiple_of(band_of(side, 2 * i) * LATS, 16)
            table.append(pltpu.make_async_copy(
                legendre_hbm.at[0, pl.ds(at, PAIR)], legendre.at[pl.ds(row, PAIR)], local_sem))
            at = pl.multiple_of(tail_at + TAIL * i, 16)
            table.append(pltpu.make_async_copy(
                legendre_hbm.at[0, pl.ds(at, TAIL)], legendre.at[pl.ds(row + PAIR, TAIL)], local_sem))
    for copy in table:
        copy.start()
    for copy in small:
        copy.wait()
    total = spectral.shape[1]
    wave_of_lane = lax.broadcasted_iota(jnp.int32, (128, total), 1).astype(F32)
    for t in range(total // 128):
        column = turned(waves[t:t + 1, :].astype(F32))
        chosen[128 * t:128 * (t + 1)] = jnp.where(wave_of_lane == column, 1.0, 0.0).astype(BF16)
    weight = turned(quad[...])
    fetch.wait()
    for r in range(8):
        rows = jnp.concatenate([fourier[r].astype(F32) * weight, jnp.zeros((8, total), F32)], axis=0)
        weighted[64 * r:64 * (r + 1)] = rows.astype(BF16)
    for n in range(2):
        found = lax.dot_general(
            chosen[...], weighted[256 * n:256 * (n + 1)], (((1,), (1,)), ((), ())), preferred_element_type=F32)
        gathered[2 * n] = found[:, :128]
        gathered[2 * n + 1] = found[:, 128:]

    low_lanes, body_lanes = lanes() < LATS, lanes() < PAIR

    def side_by_side(even, odd, r):
        if r % 2 == 0:
            return jnp.where(low_lanes, even, roll(odd, LATS))
        return jnp.where(low_lanes, roll(even, -64), roll(odd, LATS - 64))

    def rows_pair(t, carry):
        for half in range(2):
            start = (1 - parity + 2 * half) * NY * NF + 16 * t
            for r in range(8):
                even = gathered[r // 2, pl.ds(start, 8, stride=2), :]
                odd = gathered[r // 2, pl.ds(start + 1, 8, stride=2), :]
                at = (half * NY * NZ + 8 * t) * 8 + r
                tiles_b[pl.ds(at, 8, stride=8), :] = side_by_side(even, odd, r)
        return carry

    def rows_dense(i, carry):
        band = (parity + 2 * ((2 * i) // NY)) * NY + lax.rem(2 * i, NY)
        for t in range(NF // 8):
            start = pl.multiple_of(band * NF + 8 * t, 8)
            for r in range(8):
                even = gathered[r // 2, pl.ds(start, 8), :]
                odd = gathered[r // 2, pl.ds(pl.multiple_of(start + NF, 8), 8), :]
                at = 8 * t * SKEW + 8 * i + r
                tiles_a[pl.ds(at, 8, stride=SKEW), :] = side_by_side(even, odd, r)
        return carry

    def pack_pair(j, carry):
        for k in range(NZ):
            sb1[j, k] = tiles_b[pl.ds(pl.multiple_of((j * NZ + chip_of(z, k)) * 8, 8), 8), :].astype(BF16)
        return carry

    def pack_dense(field, carry):
        tiles = [tiles_a[pl.ds(pl.multiple_of(field * SKEW + 8 * i, 8), 8), :] for i in range(ND + 1)]
        for i in range(ND):
            sa1[field, i] = jnp.where(body_lanes, tiles[i], roll(tiles[ND], PAIR - TAIL * i)).astype(BF16)
        return carry

    lax.fori_loop(0, ND + 1, rows_dense, 0, unroll=2)
    lax.fori_loop(0, NF, pack_dense, 0, unroll=3)
    lax.fori_loop(0, NY * NZ // 8, rows_pair, 0, unroll=2)
    lax.fori_loop(0, HB, pack_pair, 0, unroll=2)
    pl.semaphore_wait(barrier, NB + NF - 2)

    def send(src, dst, phase, device):
        pltpu.make_async_remote_copy(
            src_ref=src, dst_ref=dst, send_sem=send_sem.at[phase], recv_sem=recv_sem.at[phase],
            device_id=device, device_id_type=MESH).start()

    def send_field(src, dst, phase, chunk):
        for d in Z_ORDERS[chunk]:
            for k in range(2):
                if d == 0 and k == 0:
                    continue
                to = lax.rem(z + d + NZ, NZ) * 2 + lax.rem(core + k, 2)
                send(src.at[to], dst.at[f], 2 * phase + chunk, (b, to))
        if chunk == 1:
            dst[f] = src[f]

    def send_band(src, dst, phase, chunk, same):
        part = pl.ds(*CHUNKS[chunk])
        for dy in Y_ORDER:
            for dx in (2, 0) if same else (1, 3):
                if dx == 0 and dy == 0:
                    continue
                to_x, to_y = lax.rem(x + dx, NX), lax.rem(y + dy + NY, NY)
                to = (to_x // 2) * NY + to_y
                send(src.at[to, part], dst.at[mine, part], 2 * phase + chunk, (to_x * NY + to_y, f))
        if same:
            dst[mine, part] = src[mine, part]

    def wait_some(some, phase, received):
        copy = pltpu.make_async_remote_copy(
            src_ref=some, dst_ref=some, send_sem=send_sem.at[phase], recv_sem=recv_sem.at[phase],
            device_id=(b, f), device_id_type=MESH)
        if received:
            copy.wait_recv()
        else:
            copy.wait_send()

    def wait_field(ref, phase, chunk, received=True):
        wait_some(ref.at[pl.ds(0, (10, 13)[chunk])], 2 * phase + chunk, received)

    def wait_band(ref, phase, chunk, same, received=True):
        wait_some(ref.at[pl.ds(0, HB - 1 if same else HB), pl.ds(*CHUNKS[chunk])], 2 * phase + chunk, received)

    def over_chunk(chunk, body):
        first, count = CHUNKS[chunk]

        def step(k, carry):
            body(first + k)
            return carry

        lax.fori_loop(0, count, step, 0, unroll=count)

    def put_dense(src, dst, chunk):
        def body(t):
            out = pair_to_dense(src, t)
            for c in range(2):
                for i in range(ND):
                    dst[2 * chip_of(z, t) + c, i] = out[c][i].astype(BF16)

        over_chunk(chunk, body)

    def put_pair(src, dst, chunk):
        over_chunk(chunk, functools.partial(dense_to_pair, src, dst, z))

    for chunk in range(2):
        send_field(sa1, ra1, 0, chunk)
    for chunk in range(2):
        send_band(sb1, rb1, 1, chunk, False)
    order = lax.broadcasted_iota(jnp.int32, (LEV, total), 1).astype(F32)
    gamma[...] = 1.0 / (1.0 + turned(rates[...]) * (order * (order + 1.0) / float(total * total)))
    place_of = lax.broadcasted_iota(jnp.int32, waves.shape, 0) * 128 + lax.broadcasted_iota(jnp.int32, waves.shape, 1)
    mine_only = jnp.where(place_of == b * NF + f, waves[...].astype(F32), 0.0)
    my_wave = jnp.sum(jnp.sum(mine_only, axis=1, keepdims=True), axis=0, keepdims=True)
    keep[...] = jnp.where(order[:1] >= my_wave, 1.0, 0.0)
    proj_parts[...] = jnp.concatenate(parts_of(proj[...]), axis=0)
    recon_parts[...] = jnp.concatenate(parts_of(recon[...]), axis=0)

    def second_phase(in_b, out_b, end_b, in_a, out_a, end_a, phase):
        for chunk in range(2):
            wait_band(in_b, phase + 1, chunk, False)
            put_dense(in_b, out_b, chunk)
            send_field(out_b, end_b, phase + 2, chunk)
            wait_field(in_a, phase, chunk)
            put_pair(in_a, out_a, chunk)
            send_band(out_a, end_a, phase + 3, chunk, True)

    second_phase(rb1, sb2, rb2, ra1, sa2, ra2, 0)
    for copy in table:
        copy.wait()
    step_n = 256
    half_k = ND * 128

    def left_a(t):
        out = pair_to_dense(ra2, t)
        row = pl.multiple_of(16 * chip_of(z, t), 16)
        for i in range(ND):
            both = jnp.concatenate([out[0][i], out[1][i]], axis=0)
            left[pl.ds(row, 16), 128 * i:128 * (i + 1)] = both.astype(BF16)

    for chunk in range(2):
        wait_band(ra2, 3, chunk, True)
        over_chunk(chunk, left_a)
    for n in range(0, total, step_n):
        direct[:, n:n + step_n] = jnp.dot(
            left[:, :half_k], legendre[:half_k, n:n + step_n], preferred_element_type=F32)

    for chunk in range(2):
        wait_field(rb2, 2, chunk)

    def left_b(k, carry):
        for i in range(ND):
            both = jnp.concatenate([rb2[2 * k, i].astype(F32), rb2[2 * k + 1, i].astype(F32)], axis=0)
            left[pl.ds(pl.multiple_of(16 * k, 16), 16), half_k + 128 * i:half_k + 128 * (i + 1)] = both.astype(BF16)
        return carry

    lax.fori_loop(0, NZ, left_b, 0, unroll=3)
    for n in range(0, total, step_n):
        direct[:, n:n + step_n] += jnp.dot(
            left[:, half_k:], legendre[half_k:, n:n + step_n], preferred_element_type=F32)
    pieces = [(LEV * c, n) for n in range(0, total, step_n) for c in range(2)]
    for row, n in pieces:
        found = near_exact(proj_parts[...], direct[row:row + LEV, n:n + step_n])
        modes[row:row + LEV, n:n + step_n] = gamma[:, n:n + step_n] * found
    for row, n in pieces:
        solved = near_exact(recon_parts[...], modes[row:row + LEV, n:n + step_n])
        spectral[row:row + LEV, n:n + step_n] = jnp.where(keep[:, n:n + step_n] > 0.5, solved, 0.0).astype(BF16)

    def back(part, out):
        for i in range(0, ND, 2):
            count = min(2, ND - i)
            row = (part * ND + i) * 128
            made = lax.dot_general(
                spectral[...], legendre[row:row + 128 * count, :], (((1,), (1,)), ((), ())), preferred_element_type=F32)
            for k in range(count):
                out[:, i + k] = made[:, 128 * k:128 * (k + 1)].reshape(NF, 8, 128).astype(BF16)

    back(0, xa)
    for chunk in range(2):
        send_field(xa, ya, 4, chunk)
    back(1, xb)
    for chunk in range(2):
        put_pair(xb, yb, chunk)
        send_band(yb, zb, 5, chunk, False)

    second_phase(zb, vb, last_b, ya, za, last_a, 4)
    for chunk in range(2):
        wait_band(last_a, 7, chunk, True)
    for chunk in range(2):
        wait_field(last_b, 6, chunk)
    for chunk in range(2):
        for ref, phase in ((sa1, 0), (sb2, 2), (xa, 4), (vb, 6)):
            wait_field(ref, phase, chunk, received=False)
        for ref, phase, same in ((sb1, 1, False), (sa2, 3, True), (yb, 5, False), (za, 7, True)):
            wait_band(ref, phase, chunk, same, received=False)


def place_kernel(waves, from_a, from_b, solved, returned, spectral, placed):
    spectral[...] = solved[...]
    b = lax.axis_index("band")
    parity = lax.rem(b // NY, 2)
    z = lax.axis_index("field") // 2
    lane = lanes()

    def put(band, field, tile):
        placed[pl.ds(pl.multiple_of(waves[band * NF + field] * 8, 8), 8), :] = tile

    def one_a(j, carry):
        band = (parity + 2 * (j // NY)) * NY + lax.rem(j, NY)
        for k in range(NZ):
            tile = from_a[j, k].astype(F32)
            put(band, 2 * chip_of(z, k), tile)
            put(band, 2 * chip_of(z, k) + 1, roll(tile, -LATS))
        return carry

    lax.fori_loop(0, HB, one_a, 0, unroll=4)

    def one_b(field, carry):
        tiles = [from_b[field, i].astype(F32) for i in range(ND)]
        last = roll(tiles[0], TAIL)
        for i in range(1, ND):
            last = jnp.where(lane < TAIL * i, last, roll(tiles[i], TAIL + TAIL * i))
        for i, tile in enumerate(tiles + [last]):
            put(band_of(1 - parity, 2 * i), field, tile)
            put(band_of(1 - parity, 2 * i + 1), field, roll(tile, -LATS))
        return carry

    lax.fori_loop(0, NF, one_b, 0, unroll=4)

    total = returned.shape[2]
    rows = lax.broadcasted_iota(jnp.int32, (LATS, 128), 0)
    same = jnp.where(rows == lax.broadcasted_iota(jnp.int32, (LATS, 128), 1), 1.0, 0.0).astype(BF16)
    for r in range(8):
        waves_by_lat = placed[pl.ds(r, total, stride=8), :].astype(BF16)
        returned[r] = lax.dot_general(
            same, waves_by_lat, (((1,), (1,)), ((), ())), preferred_element_type=F32).astype(BF16)


def per_device(fourier, quad_weights, legendre, slot_wave, vert_proj, vert_recon, vert_rates):
    nlat, total = legendre.shape[1:]
    dense = (NF, ND, 8, 128)
    pair = (HB, NZ, 8, 128)
    vmem, smem = pl.BlockSpec(memory_space=pltpu.VMEM), pl.BlockSpec(memory_space=pltpu.SMEM)
    hbm = pl.BlockSpec(memory_space=pltpu.HBM)
    buffers = [dense, dense, pair, pair, pair, pair, dense, dense, dense, dense, pair, dense, pair, pair, dense]
    spectral, last_a, last_b = pl.pallas_call(
        exchange_kernel,
        out_shape=(
            jax.ShapeDtypeStruct((2 * LEV, total), BF16),
            jax.ShapeDtypeStruct(pair, BF16),
            jax.ShapeDtypeStruct(dense, BF16),
        ),
        in_specs=[hbm] * 7,
        out_specs=[vmem, vmem, vmem],
        scratch_shapes=[
            pltpu.VMEM((total // 128, 128), jnp.int32),
            pltpu.VMEM((1, LATS), F32),
            pltpu.VMEM((1, LEV), F32),
            pltpu.VMEM((LEV, LEV), F32),
            pltpu.VMEM((LEV, LEV), F32),
            pltpu.VMEM((LEV, total), F32),
            pltpu.VMEM((1, total), F32),
            pltpu.VMEM((2 * LEV, LEV), BF16),
            pltpu.VMEM((2 * LEV, LEV), BF16),
            pltpu.VMEM((2 * LEV, total), F32),
            pltpu.VMEM((nlat, total), BF16),
            pltpu.VMEM((2 * LEV, nlat), BF16),
            pltpu.VMEM((2 * LEV, total), F32),
            pltpu.VMEM((8, LATS, total), BF16),
            pltpu.VMEM((512, total), BF16),
            pltpu.VMEM((total, total), BF16),
            pltpu.VMEM((4, total, 128), F32),
            pltpu.VMEM((NF * SKEW, 128), F32),
            pltpu.VMEM((HB * NZ * 8, 128), F32),
        ]
        + [pltpu.VMEM(shape, BF16) for shape in buffers]
        + [pltpu.SemaphoreType.DMA((5,)), pltpu.SemaphoreType.DMA, pltpu.SemaphoreType.DMA, pltpu.SemaphoreType.DMA((16,)), pltpu.SemaphoreType.DMA((16,))],
        compiler_params=pltpu.CompilerParams(
            collective_id=0, has_side_effects=True, vmem_limit_bytes=55_000_000),
        name="exchange",
    )(*[pltpu.with_memory_space_constraint(v, pltpu.HBM) for v in (
        slot_wave.reshape(total // 128, 128), quad_weights.reshape(1, LATS), vert_rates.reshape(1, LEV),
        vert_proj, vert_recon, jnp.transpose(fourier, (1, 2, 0)), legendre)])
    returned, spectral = pl.pallas_call(
        place_kernel,
        out_shape=(jax.ShapeDtypeStruct((8, LATS, total), BF16), jax.ShapeDtypeStruct(spectral.shape, BF16)),
        in_specs=[smem, vmem, vmem, vmem],
        out_specs=[vmem, vmem],
        scratch_shapes=[pltpu.VMEM((total * 8, 128), F32)],
        compiler_params=pltpu.CompilerParams(vmem_limit_bytes=16 * 1024 * 1024),
        name="place",
    )(slot_wave, last_a, last_b, spectral)
    return spectral.reshape(1, 2, LEV, total), jnp.transpose(returned, (2, 0, 1))


def solution(mesh):
    placed = (
        P(None, "field", "band"),
        P("band"),
        P(("band", "field"), None, None),
        P(),
        P(),
        P(),
        P(),
    )
    return jax.shard_map(
        per_device,
        mesh=mesh,
        in_specs=placed,
        out_specs=(P(("band", "field"), None, None, None), P(None, "field", "band")),
        check_vma=False,
    )
```

```python
import functools

import jax
import jax.numpy as jnp
from jax import lax
from jax.experimental import pallas as pl
from jax.experimental.pallas import tpu as pltpu
from jax.sharding import PartitionSpec as P

MESH = pl.DeviceIdType.MESH
F32, BF16 = jnp.float32, jnp.bfloat16
LEV = 96
NX, NY, NZ = 4, 8, 12
NB, NF = NX * NY, 2 * NZ
HB = NB // 2
LATS = 56
PAIR = 2 * LATS
TAIL = 128 - PAIR
ND = HB // 2 - 1
SKEW = 8 * (ND + 1) + 8
FAR = 4
CHUNKS = ((0, 5), (5, 7))
Z_ORDERS = ((6, 5, -5, 4, -4), (3, -3, 2, -2, 1, -1, 0))
Y_ORDER = (4, 3, -3, 2, -2, 1, -1, 0)


def band_of(parity, j):
    return (parity + 2 * (j // NY)) * NY + j % NY


def lanes():
    return lax.broadcasted_iota(jnp.int32, (8, 128), 1)


def roll(v, by):
    return pltpu.roll(v, by % 128, 1)


def chip_of(z, t):
    return lax.rem(z + FAR + t, NZ)


def dense_to_pair(src, dst, z, t):
    lane = lanes()
    low = lane < LATS
    halves = []
    for core in range(2):
        f = 2 * chip_of(z, t) + core
        tiles = [src[f, i].astype(F32) for i in range(ND)]
        last = roll(tiles[0], TAIL)
        for i in range(1, ND):
            last = jnp.where(lane < TAIL * i, last, roll(tiles[i], TAIL + TAIL * i))
        halves.append(tiles + [last])
    for i in range(ND + 1):
        one, two = halves[0][i], halves[1][i]
        dst[2 * i, t] = jnp.where(low, one, roll(two, LATS)).astype(BF16)
        dst[2 * i + 1, t] = jnp.where(low, roll(one, -LATS), two).astype(BF16)


def pair_to_dense(src, t):
    lane = lanes()
    low, body = lane < LATS, lane < PAIR
    first, second = [], []
    for i in range(ND + 1):
        even, odd = src[2 * i, t].astype(F32), src[2 * i + 1, t].astype(F32)
        first.append(jnp.where(low, even, roll(odd, LATS)))
        second.append(jnp.where(low, roll(even, -LATS), odd))
    out = []
    for tiles in (first, second):
        out.append([jnp.where(body, tiles[i], roll(tiles[ND], PAIR - TAIL * i)) for i in range(ND)])
    return out


def turned(row):
    n = row.shape[1]
    diagonal = lax.broadcasted_iota(jnp.int32, (n, n), 0) == lax.broadcasted_iota(jnp.int32, (n, n), 1)
    return jnp.sum(jnp.where(diagonal, row, 0.0), axis=1, keepdims=True)


def parts_of(v):
    high = v.astype(BF16)
    return high, (v - high.astype(F32)).astype(BF16)


def near_exact(left, right):
    n = left.shape[0] // 2
    high, low = parts_of(right)
    both = jnp.dot(left, high, preferred_element_type=F32)
    return both[:n] + (both[n:] + jnp.dot(left[:n], low, preferred_element_type=F32))


def exchange_kernel(
    waves_hbm, quad_hbm, rates_hbm, proj_hbm, recon_hbm, fourier_hbm, legendre_hbm,
    spectral, last_a, last_b,
    waves, quad, rates, proj, recon, gamma, keep, proj_parts, recon_parts, modes,
    legendre, left, direct, fourier, weighted, chosen, gathered, tiles_a, tiles_b,
    sa1, ra1, sa2, ra2, sb1, rb1, sb2, rb2,
    xa, ya, za, xb, yb, zb, vb,
    small_sem, local_sem, fetch_sem, send_sem, recv_sem,
):
    b, f = lax.axis_index("band"), lax.axis_index("field")
    x, y = b // NY, lax.rem(b, NY)
    z, core = f // 2, lax.rem(f, 2)
    parity, mine = lax.rem(x, 2), (x // 2) * NY + y

    barrier = pltpu.get_barrier_semaphore()

    small = [
        pltpu.make_async_copy(src, dst, small_sem.at[i])
        for i, (src, dst) in enumerate(
            ((waves_hbm, waves), (quad_hbm, quad), (rates_hbm, rates), (proj_hbm, proj), (recon_hbm, recon)))]
    fetch = pltpu.make_async_copy(fourier_hbm, fourier, fetch_sem)
    for copy in small:
        copy.start()
    fetch.start()

    greeted = [(abs(d), "field", d, k) for order in Z_ORDERS for d in order for k in range(2) if (d, k) != (0, 0)]
    greeted += [
        (min(dx, NX - dx) + abs(dy), "band", dx, dy) for dy in Y_ORDER for dx in range(NX) if (dx, dy) != (0, 0)]
    for _, axis, one, two in sorted(greeted, key=lambda item: -item[0]):
        if axis == "field":
            to = (b, lax.rem(z + one + NZ, NZ) * 2 + lax.rem(core + two, 2))
        else:
            to = (lax.rem(x + one, NX) * NY + lax.rem(y + two + NY, NY), f)
        pl.semaphore_signal(barrier, 1, device_id=to, device_id_type=MESH)

    table = []
    for part in range(2):
        side = parity if part == 0 else 1 - parity
        tail_at = band_of(side, HB - 2) * LATS
        for i in range(ND):
            row = (part * ND + i) * 128
            at = pl.multiple_of(band_of(side, 2 * i) * LATS, 16)
            table.append(pltpu.make_async_copy(
                legendre_hbm.at[0, pl.ds(at, PAIR)], legendre.at[pl.ds(row, PAIR)], local_sem))
            at = pl.multiple_of(tail_at + TAIL * i, 16)
            table.append(pltpu.make_async_copy(
                legendre_hbm.at[0, pl.ds(at, TAIL)], legendre.at[pl.ds(row + PAIR, TAIL)], local_sem))
    for copy in table:
        copy.start()
    for copy in small:
        copy.wait()
    total = spectral.shape[1]
    wave_of_lane = lax.broadcasted_iota(jnp.int32, (128, total), 1).astype(F32)
    for t in range(total // 128):
        column = turned(waves[t:t + 1, :].astype(F32))
        chosen[128 * t:128 * (t + 1)] = jnp.where(wave_of_lane == column, 1.0, 0.0).astype(BF16)
    weight = turned(quad[...])
    fetch.wait()
    for r in range(8):
        rows = jnp.concatenate([fourier[r].astype(F32) * weight, jnp.zeros((8, total), F32)], axis=0)
        weighted[64 * r:64 * (r + 1)] = rows.astype(BF16)
    for n in range(2):
        found = lax.dot_general(
            chosen[...], weighted[256 * n:256 * (n + 1)], (((1,), (1,)), ((), ())), preferred_element_type=F32)
        gathered[2 * n] = found[:, :128]
        gathered[2 * n + 1] = found[:, 128:]

    low_lanes, body_lanes = lanes() < LATS, lanes() < PAIR

    def side_by_side(even, odd, r):
        if r % 2 == 0:
            return jnp.where(low_lanes, even, roll(odd, LATS))
        return jnp.where(low_lanes, roll(even, -64), roll(odd, LATS - 64))

    def rows_pair(t, carry):
        for half in range(2):
            start = (1 - parity + 2 * half) * NY * NF + 16 * t
            for r in range(8):
                even = gathered[r // 2, pl.ds(start, 8, stride=2), :]
                odd = gathered[r // 2, pl.ds(start + 1, 8, stride=2), :]
                at = (half * NY * NZ + 8 * t) * 8 + r
                tiles_b[pl.ds(at, 8, stride=8), :] = side_by_side(even, odd, r)
        return carry

    def rows_dense(i, carry):
        band = (parity + 2 * ((2 * i) // NY)) * NY + lax.rem(2 * i, NY)
        for t in range(NF // 8):
            start = pl.multiple_of(band * NF + 8 * t, 8)
            for r in range(8):
                even = gathered[r // 2, pl.ds(start, 8), :]
                odd = gathered[r // 2, pl.ds(pl.multiple_of(start + NF, 8), 8), :]
                at = 8 * t * SKEW + 8 * i + r
                tiles_a[pl.ds(at, 8, stride=SKEW), :] = side_by_side(even, odd, r)
        return carry

    def pack_pair(j, carry):
        for k in range(NZ):
            sb1[j, k] = tiles_b[pl.ds(pl.multiple_of((j * NZ + chip_of(z, k)) * 8, 8), 8), :].astype(BF16)
        return carry

    def pack_dense(field, carry):
        tiles = [tiles_a[pl.ds(pl.multiple_of(field * SKEW + 8 * i, 8), 8), :] for i in range(ND + 1)]
        for i in range(ND):
            sa1[field, i] = jnp.where(body_lanes, tiles[i], roll(tiles[ND], PAIR - TAIL * i)).astype(BF16)
        return carry

    lax.fori_loop(0, ND + 1, rows_dense, 0, unroll=2)
    lax.fori_loop(0, NF, pack_dense, 0, unroll=3)
    lax.fori_loop(0, NY * NZ // 8, rows_pair, 0, unroll=2)
    lax.fori_loop(0, HB, pack_pair, 0, unroll=2)
    pl.semaphore_wait(barrier, NB + NF - 2)

    def send(src, dst, phase, device):
        pltpu.make_async_remote_copy(
            src_ref=src, dst_ref=dst, send_sem=send_sem.at[phase], recv_sem=recv_sem.at[phase],
            device_id=device, device_id_type=MESH).start()

    def send_field(src, dst, phase, chunk):
        for d in Z_ORDERS[chunk]:
            for k in range(2):
                if d == 0 and k == 0:
                    continue
                to = lax.rem(z + d + NZ, NZ) * 2 + lax.rem(core + k, 2)
                send(src.at[to], dst.at[f], 2 * phase + chunk, (b, to))
        if chunk == 1:
            dst[f] = src[f]

    def send_band(src, dst, phase, chunk, same):
        part = pl.ds(*CHUNKS[chunk])
        for dy in Y_ORDER:
            for dx in (2, 0) if same else (1, 3):
                if dx == 0 and dy == 0:
                    continue
                to_x, to_y = lax.rem(x + dx, NX), lax.rem(y + dy + NY, NY)
                to = (to_x // 2) * NY + to_y
                send(src.at[to, part], dst.at[mine, part], 2 * phase + chunk, (to_x * NY + to_y, f))
        if same:
            dst[mine, part] = src[mine, part]

    def wait_some(some, phase, received):
        copy = pltpu.make_async_remote_copy(
            src_ref=some, dst_ref=some, send_sem=send_sem.at[phase], recv_sem=recv_sem.at[phase],
            device_id=(b, f), device_id_type=MESH)
        if received:
            copy.wait_recv()
        else:
            copy.wait_send()

    def wait_field(ref, phase, chunk, received=True):
        wait_some(ref.at[pl.ds(0, (10, 13)[chunk])], 2 * phase + chunk, received)

    def wait_band(ref, phase, chunk, same, received=True):
        wait_some(ref.at[pl.ds(0, HB - 1 if same else HB), pl.ds(*CHUNKS[chunk])], 2 * phase + chunk, received)

    def over_chunk(chunk, body):
        first, count = CHUNKS[chunk]

        def step(k, carry):
            body(first + k)
            return carry

        lax.fori_loop(0, count, step, 0, unroll=count)

    def put_dense(src, dst, chunk):
        def body(t):
            out = pair_to_dense(src, t)
            for c in range(2):
                for i in range(ND):
                    dst[2 * chip_of(z, t) + c, i] = out[c][i].astype(BF16)

        over_chunk(chunk, body)

    def put_pair(src, dst, chunk):
        over_chunk(chunk, functools.partial(dense_to_pair, src, dst, z))

    for chunk in range(2):
        send_field(sa1, ra1, 0, chunk)
    for chunk in range(2):
        send_band(sb1, rb1, 1, chunk, False)
    order = lax.broadcasted_iota(jnp.int32, (LEV, total), 1).astype(F32)
    gamma[...] = 1.0 / (1.0 + turned(rates[...]) * (order * (order + 1.0) / float(total * total)))
    place_of = lax.broadcasted_iota(jnp.int32, waves.shape, 0) * 128 + lax.broadcasted_iota(jnp.int32, waves.shape, 1)
    mine_only = jnp.where(place_of == b * NF + f, waves[...].astype(F32), 0.0)
    my_wave = jnp.sum(jnp.sum(mine_only, axis=1, keepdims=True), axis=0, keepdims=True)
    keep[...] = jnp.where(order[:1] >= my_wave, 1.0, 0.0)
    proj_parts[...] = jnp.concatenate(parts_of(proj[...]), axis=0)
    recon_parts[...] = jnp.concatenate(parts_of(recon[...]), axis=0)

    def second_phase(in_b, out_b, end_b, in_a, out_a, end_a, phase):
        for chunk in range(2):
            wait_band(in_b, phase + 1, chunk, False)
            put_dense(in_b, out_b, chunk)
            send_field(out_b, end_b, phase + 2, chunk)
            wait_field(in_a, phase, chunk)
            put_pair(in_a, out_a, chunk)
            send_band(out_a, end_a, phase + 3, chunk, True)

    second_phase(rb1, sb2, rb2, ra1, sa2, ra2, 0)
    for copy in table:
        copy.wait()
    step_n = 256
    half_k = ND * 128

    def left_a(t):
        out = pair_to_dense(ra2, t)
        row = pl.multiple_of(16 * chip_of(z, t), 16)
        for i in range(ND):
            both = jnp.concatenate([out[0][i], out[1][i]], axis=0)
            left[pl.ds(row, 16), 128 * i:128 * (i + 1)] = both.astype(BF16)

    for chunk in range(2):
        wait_band(ra2, 3, chunk, True)
        over_chunk(chunk, left_a)
    for n in range(0, total, step_n):
        direct[:, n:n + step_n] = jnp.dot(
            left[:, :half_k], legendre[:half_k, n:n + step_n], preferred_element_type=F32)

    for chunk in range(2):
        wait_field(rb2, 2, chunk)

    def left_b(k, carry):
        for i in range(ND):
            both = jnp.concatenate([rb2[2 * k, i].astype(F32), rb2[2 * k + 1, i].astype(F32)], axis=0)
            left[pl.ds(pl.multiple_of(16 * k, 16), 16), half_k + 128 * i:half_k + 128 * (i + 1)] = both.astype(BF16)
        return carry

    lax.fori_loop(0, NZ, left_b, 0, unroll=3)
    for n in range(0, total, step_n):
        direct[:, n:n + step_n] += jnp.dot(
            left[:, half_k:], legendre[half_k:, n:n + step_n], preferred_element_type=F32)
    pieces = [(LEV * c, n) for n in range(0, total, step_n) for c in range(2)]
    for row, n in pieces:
        found = near_exact(proj_parts[...], direct[row:row + LEV, n:n + step_n])
        modes[row:row + LEV, n:n + step_n] = gamma[:, n:n + step_n] * found
    for row, n in pieces:
        solved = near_exact(recon_parts[...], modes[row:row + LEV, n:n + step_n])
        spectral[row:row + LEV, n:n + step_n] = jnp.where(keep[:, n:n + step_n] > 0.5, solved, 0.0).astype(BF16)

    def back(part, out):
        for i in range(0, ND, 2):
            count = min(2, ND - i)
            row = (part * ND + i) * 128
            made = lax.dot_general(
                spectral[...], legendre[row:row + 128 * count, :], (((1,), (1,)), ((), ())), preferred_element_type=F32)
            for k in range(count):
                out[:, i + k] = made[:, 128 * k:128 * (k + 1)].reshape(NF, 8, 128).astype(BF16)

    back(0, xa)
    for chunk in range(2):
        send_field(xa, ya, 4, chunk)
    back(1, xb)
    for chunk in range(2):
        put_pair(xb, yb, chunk)
        send_band(yb, zb, 5, chunk, False)

    second_phase(zb, vb, last_b, ya, za, last_a, 4)
    for chunk in range(2):
        wait_band(last_a, 7, chunk, True)
    for chunk in range(2):
        wait_field(last_b, 6, chunk)
    for chunk in range(2):
        for ref, phase in ((sa1, 0), (sb2, 2), (xa, 4), (vb, 6)):
            wait_field(ref, phase, chunk, received=False)
        for ref, phase, same in ((sb1, 1, False), (sa2, 3, True), (yb, 5, False), (za, 7, True)):
            wait_band(ref, phase, chunk, same, received=False)


def place_kernel(waves, from_a, from_b, solved, returned, spectral, placed, made, out_sem):
    copies = [pltpu.make_async_copy(solved, spectral, out_sem.at[8])]
    copies[0].start()
    b = lax.axis_index("band")
    parity = lax.rem(b // NY, 2)
    z = lax.axis_index("field") // 2
    lane = lanes()

    def put(band, field, tile):
        placed[pl.ds(pl.multiple_of(waves[band * NF + field] * 8, 8), 8), :] = tile

    fields = [2 * chip_of(z, k) for k in range(NZ)]

    def one_a(j, carry):
        band = (parity + 2 * (j // NY)) * NY + lax.rem(j, NY)
        for k in range(NZ):
            tile = from_a[j, k].astype(F32)
            put(band, fields[k], tile)
            put(band, fields[k] + 1, roll(tile, -LATS))
        return carry

    lax.fori_loop(0, HB, one_a, 0, unroll=8)

    def one_b(field, carry):
        tiles = [from_b[field, i].astype(F32) for i in range(ND)]
        last = roll(tiles[0], TAIL)
        for i in range(1, ND):
            last = jnp.where(lane < TAIL * i, last, roll(tiles[i], TAIL + TAIL * i))
        for i, tile in enumerate(tiles + [last]):
            put(band_of(1 - parity, 2 * i), field, tile)
            put(band_of(1 - parity, 2 * i + 1), field, roll(tile, -LATS))
        return carry

    lax.fori_loop(0, NF, one_b, 0, unroll=8)

    total = returned.shape[2]
    rows = lax.broadcasted_iota(jnp.int32, (LATS, 128), 0)
    same = jnp.where(rows == lax.broadcasted_iota(jnp.int32, (LATS, 128), 1), 1.0, 0.0).astype(BF16)
    for r in range(8):
        waves_by_lat = placed[pl.ds(r, total, stride=8), :].astype(BF16)
        made[r] = lax.dot_general(
            same, waves_by_lat, (((1,), (1,)), ((), ())), preferred_element_type=F32).astype(BF16)
        copies.append(pltpu.make_async_copy(made.at[r], returned.at[r], out_sem.at[r]))
        copies[-1].start()
    for copy in copies:
        copy.wait()


def per_device(fourier, quad_weights, legendre, slot_wave, vert_proj, vert_recon, vert_rates):
    nlat, total = legendre.shape[1:]
    dense = (NF, ND, 8, 128)
    pair = (HB, NZ, 8, 128)
    vmem, smem = pl.BlockSpec(memory_space=pltpu.VMEM), pl.BlockSpec(memory_space=pltpu.SMEM)
    hbm = pl.BlockSpec(memory_space=pltpu.HBM)
    buffers = [dense, dense, pair, pair, pair, pair, dense, dense, dense, dense, pair, dense, pair, pair, dense]
    spectral, last_a, last_b = pl.pallas_call(
        exchange_kernel,
        out_shape=(
            jax.ShapeDtypeStruct((2 * LEV, total), BF16),
            jax.ShapeDtypeStruct(pair, BF16),
            jax.ShapeDtypeStruct(dense, BF16),
        ),
        in_specs=[hbm] * 7,
        out_specs=[vmem, vmem, vmem],
        scratch_shapes=[
            pltpu.VMEM((total // 128, 128), jnp.int32),
            pltpu.VMEM((1, LATS), F32),
            pltpu.VMEM((1, LEV), F32),
            pltpu.VMEM((LEV, LEV), F32),
            pltpu.VMEM((LEV, LEV), F32),
            pltpu.VMEM((LEV, total), F32),
            pltpu.VMEM((1, total), F32),
            pltpu.VMEM((2 * LEV, LEV), BF16),
            pltpu.VMEM((2 * LEV, LEV), BF16),
            pltpu.VMEM((2 * LEV, total), F32),
            pltpu.VMEM((nlat, total), BF16),
            pltpu.VMEM((2 * LEV, nlat), BF16),
            pltpu.VMEM((2 * LEV, total), F32),
            pltpu.VMEM((8, LATS, total), BF16),
            pltpu.VMEM((512, total), BF16),
            pltpu.VMEM((total, total), BF16),
            pltpu.VMEM((4, total, 128), F32),
            pltpu.VMEM((NF * SKEW, 128), F32),
            pltpu.VMEM((HB * NZ * 8, 128), F32),
        ]
        + [pltpu.VMEM(shape, BF16) for shape in buffers]
        + [pltpu.SemaphoreType.DMA((5,)), pltpu.SemaphoreType.DMA, pltpu.SemaphoreType.DMA, pltpu.SemaphoreType.DMA((16,)), pltpu.SemaphoreType.DMA((16,))],
        compiler_params=pltpu.CompilerParams(
            collective_id=0, has_side_effects=True, vmem_limit_bytes=55_000_000),
        name="exchange",
    )(*[pltpu.with_memory_space_constraint(v, pltpu.HBM) for v in (
        slot_wave.reshape(total // 128, 128), quad_weights.reshape(1, LATS), vert_rates.reshape(1, LEV),
        vert_proj, vert_recon, jnp.transpose(fourier, (1, 2, 0)), legendre)])
    returned, spectral = pl.pallas_call(
        place_kernel,
        out_shape=(jax.ShapeDtypeStruct((8, LATS, total), BF16), jax.ShapeDtypeStruct(spectral.shape, BF16)),
        in_specs=[smem, vmem, vmem, vmem],
        out_specs=[hbm, hbm],
        scratch_shapes=[
            pltpu.VMEM((total * 8, 128), F32), pltpu.VMEM((8, LATS, total), BF16), pltpu.SemaphoreType.DMA((9,))],
        compiler_params=pltpu.CompilerParams(vmem_limit_bytes=16 * 1024 * 1024),
        name="place",
    )(slot_wave, last_a, last_b, spectral)
    return spectral.reshape(1, 2, LEV, total), jnp.transpose(returned, (2, 0, 1))


def solution(mesh):
    placed = (
        P(None, "field", "band"),
        P("band"),
        P(("band", "field"), None, None),
        P(),
        P(),
        P(),
        P(),
    )
    return jax.shard_map(
        per_device,
        mesh=mesh,
        in_specs=placed,
        out_specs=(P(("band", "field"), None, None, None), P(None, "field", "band")),
        check_vma=False,
    )
```
